256 devices in a mesh: seq: 32 (over x, y, core), tp: 8 (over z).
Axes of the slice: x: 4, y: 4, z: 8, core: 2. Of those that a mesh axis runs over, the one named last changes fastest.
Arguments:
- x_input: bfloat16 [32768, 8192], P('seq', 'tp'), may hold values from -6 to 6
- bc_input: bfloat16 [32768, 2048], P('seq', 'tp'), may hold values from -3 to 3
- z_gate: bfloat16 [32768, 8192], P('seq', 'tp'), may hold values from -6 to 6
- dt_input: bfloat16 [128, 32768], P('tp', 'seq'), may hold values from -3.4 to 3.4
- conv_weight_x: bfloat16 [4, 8192], P(None, 'tp'), may hold values from -3 to 3
- conv_weight_bc: bfloat16 [4, 2048], P(None, 'tp'), may hold values from -3 to 3
- conv_bias_x: float32 [8192], P('tp'), may hold values from -3 to 3
- conv_bias_bc: float32 [2048], P('tp'), may hold values from -3 to 3
- dt_bias: float32 [128], P('tp'), may hold values from -1 to 0.5
- decay_log: float32 [128], P('tp'), may hold values from -12 to -3.3
- skip_scale: float32 [128], P('tp'), may hold values from 0.5 to 2
- norm_gain: float32 [8192], P('tp'), may hold values from 0.25 to 1.75
Outputs:
- layer_out: bfloat16 [32768, 8192], P('seq', 'tp')
The draws below stay inside these ranges and needn't reach their ends.
All inputs are finite; a program needn't handle non-finite values.
Results may differ from the reference program's by a relative error of at most 0.0048.
Values may be sent and summed in bfloat16 or wider, within the bound.
No kernel may reach another device: no remote copies, remote signals or barrier semaphores. Data moves between devices by JAX's collectives and lax.ppermute only.
A program may use at most 64 MiB of HBM per device.

```python
import jax
import jax.numpy as jnp
from jax import lax

HEADS = 128
HEAD_DIM = 64
STATE = 128
GROUPS = 8
SPAN = 256
TOK_DEV = 1024
DI = 8192
LENGTH = 32768


def smooth_rows(key, rows, cols, knot):
    shift_key, knot_key = jax.random.split(key)
    count = rows // knot + 2
    knots = jax.random.normal(knot_key, (count, cols), dtype=jnp.float32)
    frac = (jnp.arange(knot, dtype=jnp.float32) / knot)[None, :, None]
    field = (knots[:-1][:, None, :] * (1.0 - frac) + knots[1:][:, None, :] * frac).reshape((count - 1) * knot, cols)
    offset = jax.random.randint(shift_key, (), 0, knot)
    return lax.dynamic_slice_in_dim(field, offset, rows, 0)


def draw_x_input(key, part):
    noise_key, field_key = jax.random.split(jax.random.fold_in(key, 7))
    field = smooth_rows(field_key, LENGTH, DI, SPAN)
    noise = 0.6 * jax.random.normal(noise_key, (LENGTH, DI))
    total = noise + 0.9 * field
    return jnp.clip(total, -6.0, 6.0).astype(jnp.float32).astype(jnp.bfloat16)


def draw_bc_input(key, part):
    noise_key, field_key = jax.random.split(jax.random.fold_in(key, 11))
    width = 2 * GROUPS * STATE
    field = smooth_rows(field_key, LENGTH, width, SPAN)
    noise = 0.3 * jax.random.normal(noise_key, (LENGTH, width))
    total = noise + 0.5 * field
    return jnp.clip(total, -3.0, 3.0).astype(jnp.float32).astype(jnp.bfloat16)


def draw_dt_input(key, part):
    noise_key, shift_key = jax.random.split(jax.random.fold_in(key, 23))
    blocks = LENGTH // TOK_DEV
    offsets = jax.random.uniform(shift_key, (HEADS, blocks, 1), minval=-0.8, maxval=0.8)
    noise = jnp.clip(0.5 * jax.random.normal(noise_key, (HEADS, blocks, TOK_DEV)), -2.5, 2.5)
    return (offsets + noise).reshape(HEADS, LENGTH).astype(jnp.float32).astype(jnp.bfloat16)


def draw_decay_log(key, part):
    kind_key, slow_key, other_key = jax.random.split(jax.random.fold_in(key, 41), 3)
    picker = jax.random.uniform(kind_key, (HEADS,))
    slow_heads = picker < 0.5
    slow_log = jax.random.uniform(slow_key, (HEADS,), minval=jnp.log(0.3), maxval=jnp.log(2.0)) - jnp.log(1.0 * LENGTH)
    other_log = jax.random.uniform(other_key, (HEADS,), minval=jnp.log(2.0 / LENGTH), maxval=jnp.log(1.0 / 30.0))
    return jnp.where(slow_heads, slow_log, other_log).astype(jnp.float32)


def block_scale(stream_key, shape, cuts, smallest, largest):
    level, own = 1.0, jax.random.fold_in(stream_key, 6)
    for position, blocks in cuts:
        draws = jnp.exp(jax.random.uniform(jax.random.fold_in(own, position), (blocks,), jnp.float32, smallest / len(cuts), largest / len(cuts)))
        level = level * jnp.repeat(draws, shape[position] // blocks).reshape([-1 if axis == position else 1 for axis in range(len(shape))])
    return level


def gaussian(own_key, dims, scale, bound, cuts=(), kind=jnp.bfloat16):
    entries = jax.random.normal(own_key, dims, jnp.float32) * scale
    if len(cuts) > 0:
        entries = block_scale(own_key, dims, cuts, -0.22, 0.18) * entries
    return jnp.clip(entries, min=-bound, max=bound).astype(kind)


def setup_inputs(seed: int = 0) -> dict:
    streams_of = jax.random.split(jax.random.key(seed), 13)
    x_input = draw_x_input(jax.random.fold_in(streams_of[12], 71), 0)
    bc_input = draw_bc_input(jax.random.fold_in(streams_of[12], 71), 0)
    z_gate = gaussian(streams_of[2], (LENGTH, DI), 1.0, 6.0, ((0, 32), (1, 8)))
    dt_input = draw_dt_input(jax.random.fold_in(streams_of[12], 71), 0)
    conv_weight_x = gaussian(streams_of[4], (4, DI), 4 ** -0.5, 3.0, ((1, 8),))
    conv_weight_bc = gaussian(streams_of[5], (4, 2 * GROUPS * STATE), 4 ** -0.5, 3.0, ((1, 8),))
    conv_bias_x = gaussian(streams_of[6], (DI,), 0.5, 3.0, ((0, 8),), jnp.float32)
    conv_bias_bc = gaussian(streams_of[7], (2 * GROUPS * STATE,), 0.5, 3.0, ((0, 8),), jnp.float32)
    dt_bias = jnp.clip(-1.0 + 1.5 * jax.random.uniform(streams_of[8], (HEADS,), jnp.float32) ** block_scale(streams_of[8], (HEADS,), ((0, 8),), -0.2, 0.2), -1.0, 0.5)
    decay_log = draw_decay_log(jax.random.fold_in(streams_of[12], 71), 0)
    skip_scale = jnp.clip(0.5 + 1.5 * jax.random.uniform(streams_of[10], (HEADS,), jnp.float32) ** block_scale(streams_of[10], (HEADS,), ((0, 8),), -0.2, 0.2), 0.5, 2.0)
    norm_gain = jnp.clip(1.0 + 0.15 * jax.random.normal(streams_of[11], (DI,), jnp.float32), 0.25, 1.75)
    return {"x_input": x_input, "bc_input": bc_input, "z_gate": z_gate, "dt_input": dt_input, "conv_weight_x": conv_weight_x, "conv_weight_bc": conv_weight_bc, "conv_bias_x": conv_bias_x, "conv_bias_bc": conv_bias_bc, "dt_bias": dt_bias, "decay_log": decay_log, "skip_scale": skip_scale, "norm_gain": norm_gain}


epsilon = 1e-05

def causal_conv(padded, weight, bias_row):
    length = padded.shape[0] - 3
    total = jnp.zeros((length, padded.shape[1]), jnp.float32) + bias_row.astype(jnp.float32)[None, :]
    for offset in range(4):
        total = total + padded[offset:offset + length].astype(jnp.float32) * weight[offset].astype(jnp.float32)[None, :]
    return jax.nn.silu(total).astype(jnp.bfloat16)

def span_local(x_block, bc_block, dt_block, decay_block):
    block_len = x_block.shape[0]
    heads = x_block.shape[1]
    groups = bc_block.shape[1]
    group_heads = heads // groups
    cum_decay = jnp.cumsum(decay_block, axis=1)
    b_part = bc_block[:, :, 0, :].astype(jnp.float32)
    c_part = bc_block[:, :, 1, :].astype(jnp.float32)
    scores = jnp.einsum('ign,jgn->gij', c_part, b_part)
    causal = jnp.arange(block_len)[:, None] >= jnp.arange(block_len)[None, :]
    spread = jnp.where(causal[None], cum_decay[:, :, None] - cum_decay[:, None, :], -jnp.inf)
    weights = jnp.exp(spread) * dt_block[:, None, :]
    mixing = (weights.reshape(groups, group_heads, block_len, block_len) * scores[:, None]).reshape(heads, block_len, block_len).astype(jnp.bfloat16)
    mixing = lax.optimization_barrier(mixing)
    y_intra = jnp.einsum('hij,jhp->ihp', mixing.astype(jnp.float32), x_block.astype(jnp.float32))
    to_end = jnp.exp(cum_decay[:, -1:] - cum_decay) * dt_block
    weighted = (to_end.reshape(groups, group_heads, block_len)[:, :, :, None] * b_part.transpose(1, 0, 2)[:, None]).reshape(heads, block_len, b_part.shape[2]).astype(jnp.bfloat16)
    weighted = lax.optimization_barrier(weighted)
    span_state = jnp.einsum('hjn,jhp->hnp', weighted.astype(jnp.float32), x_block.astype(jnp.float32))
    return (y_intra, span_state, cum_decay)

def state_out(c_part, cum_decay, start):
    groups = c_part.shape[1]
    heads = start.shape[0]
    grouped = start.reshape(groups, heads // groups, start.shape[1], start.shape[2])
    product = jnp.einsum('ign,grnp->igrp', c_part.astype(jnp.float32), grouped.astype(jnp.float32))
    product = product.reshape(c_part.shape[0], heads, start.shape[2])
    return jnp.exp(cum_decay).T[:, :, None] * product

def reference(x_input, bc_input, z_gate, dt_input, conv_weight_x, conv_weight_bc, conv_bias_x, conv_bias_bc, dt_bias, decay_log, skip_scale, norm_gain):
    x_conv = causal_conv(jnp.concatenate([jnp.zeros((3, x_input.shape[1]), x_input.dtype), x_input], 0), conv_weight_x, conv_bias_x)
    bc_conv = causal_conv(jnp.concatenate([jnp.zeros((3, bc_input.shape[1]), bc_input.dtype), bc_input], 0), conv_weight_bc, conv_bias_bc)
    step_size = jax.nn.softplus(dt_input.astype(jnp.float32) + dt_bias[:, None])
    log_decay = -jnp.exp(decay_log)[:, None] * step_size
    blocks = LENGTH // SPAN
    x_blocks = x_conv.reshape(blocks, SPAN, HEADS, HEAD_DIM)
    bc_blocks = bc_conv.reshape(blocks, SPAN, GROUPS, 2, STATE)
    dt_blocks = step_size.reshape(HEADS, blocks, SPAN).transpose(1, 0, 2)
    decay_blocks = log_decay.reshape(HEADS, blocks, SPAN).transpose(1, 0, 2)

    def advance(carried, pieces):
        x_block, bc_block, dt_block, decay_block = pieces
        y_intra, span_state, cum_decay = span_local(x_block, bc_block, dt_block, decay_block)
        start = lax.optimization_barrier(carried.astype(jnp.bfloat16))
        mixed_block = y_intra + state_out(bc_block[:, :, 1, :], cum_decay, start)
        carried = jnp.exp(cum_decay[:, -1])[:, None, None] * carried + span_state
        return (carried, mixed_block)
    initial = jnp.zeros((HEADS, STATE, HEAD_DIM), jnp.float32)
    _, mixed = lax.scan(advance, initial, (x_blocks, bc_blocks, dt_blocks, decay_blocks))
    mixed = mixed.reshape(LENGTH, HEADS, HEAD_DIM) + skip_scale[None, :, None] * x_conv.reshape(LENGTH, HEADS, HEAD_DIM).astype(jnp.float32)
    gated = mixed.reshape(LENGTH, DI) * jax.nn.silu(z_gate.astype(jnp.float32))
    mean_square = lax.optimization_barrier(jnp.mean(gated * gated, axis=1))
    return (gated * lax.rsqrt(mean_square + epsilon)[:, None] * norm_gain[None, :]).astype(jnp.bfloat16)
```

```python
import functools

import jax
import jax.numpy as jnp
from jax import lax
from jax.experimental import pallas as pl
from jax.experimental.pallas import tpu as pltpu
from jax.sharding import PartitionSpec as P

HEAD_DIM = 64
STATE = 128
SPAN = 256
DI = 8192
EPSILON = 1e-05

F32 = jnp.float32
BF16 = jnp.bfloat16


def column_of(scalars, count):
    rows = lax.broadcasted_iota(jnp.int32, (count, 128), 0)
    column = jnp.zeros((count, 128), F32)
    for head in range(count):
        column = jnp.where(rows == head, scalars[head], column)
    return column


def head_mask(heads, width):
    row = lax.broadcasted_iota(jnp.int32, (heads, width), 0)
    lane = lax.broadcasted_iota(jnp.int32, (heads, width), 1)
    return lane // HEAD_DIM == row


def expander(heads, width):
    one_hot = jnp.where(head_mask(heads, width), 1.0, 0.0)
    return jnp.concatenate([one_hot, one_hot], 0).astype(BF16)


def high_low(value):
    high = value.astype(BF16).astype(F32)
    return jnp.concatenate([high, value - high], 0).astype(BF16)


def spread(pair, one_hot):
    return lax.dot_general(pair, one_hot, (((0,), (0,)), ((), ())), preferred_element_type=F32)


def half_silu(half):
    return half + half * jnp.tanh(half)


def conv_tile(slab, tile, x_tile, halo_tile, weight, bias):
    rows = x_tile.shape[0]
    slab[tile, 0:8, :] = halo_tile.astype(F32)
    slab[tile, 8 : 8 + rows, :] = x_tile.astype(F32)
    total = bias
    for tap in range(4):
        total = total + slab[tile, 5 + tap : 5 + tap + rows, :] * weight[tap : tap + 1, :]
    return half_silu(total).astype(BF16)


def block_state(slab, halo_x, halo_bc, x, bc, cwx, cwbc, cbx, cbbc, pair, xc_out, xw_out, bc_out):
    width = x.shape[1]
    heads = width // HEAD_DIM
    tiles = width // 128
    for tile in range(2):
        at = slice(tile * 128, tile * 128 + 128)
        bc_out[:, at] = conv_tile(
            slab,
            tiles + tile,
            bc[:, at],
            halo_bc[:, at],
            cwbc[:, at].astype(F32) * 0.5,
            cbbc[:, at] * 0.5,
        )
    weight = spread(pair, expander(heads, width))
    for tile in range(tiles):
        at = slice(tile * 128, tile * 128 + 128)
        conv = conv_tile(
            slab, tile, x[:, at], halo_x[:, at], cwx[:, at].astype(F32) * 0.5, cbx[:, at] * 0.5
        )
        xc_out[:, at] = conv
        xw_out[:, at] = (conv.astype(F32) * weight[:, at]).astype(BF16)
    return lax.dot_general(
        bc_out[:, 0:STATE], xw_out[...], (((0,), (0,)), ((), ())), preferred_element_type=F32
    )


def first_kernel(
    x_ref, halo_x_ref, bc_ref, halo_bc_ref, dt_ref, cwx_ref, cwbc_ref, cbx_ref, cbbc_ref,
    dt_bias_ref, decay_ref,
    xc_ref, xw_ref, bcv_ref, w_ref, p_ref, pdev_ref, total_ref, state_ref,
    slab, whole,
):
    step = pl.program_id(0)
    heads, tokens = dt_ref.shape
    width = x_ref.shape[1]
    blocks = tokens // SPAN

    @pl.when(step == 0)
    def _():
        repeat = tokens // 128
        bias = jnp.concatenate([column_of(dt_bias_ref, heads)] * repeat, 1)
        rate = jnp.concatenate([jnp.exp(column_of(decay_ref, heads))] * repeat, 1)
        raw = dt_ref[...].astype(F32) + bias
        size = jnp.maximum(raw, 0.0) + jnp.log(1.0 + jnp.exp(-jnp.abs(raw)))
        cum = -rate * size
        position = lax.broadcasted_iota(jnp.int32, (heads, tokens), 1) & (SPAN - 1)
        shift = 1
        while shift < SPAN:
            cum = cum + jnp.where(position >= shift, pltpu.roll(cum, shift, 1), 0.0)
            shift *= 2
        w_ref[...] = high_low(jnp.exp(-cum) * size)
        p_ref[...] = high_low(jnp.exp(cum))
        mask = head_mask(heads, width)
        before = jnp.zeros((heads, 1), F32)
        rows = []
        for block in range(blocks):
            at = slice(block * SPAN, block * SPAN + SPAN)
            last = cum[:, block * SPAN + SPAN - 1 : block * SPAN + SPAN]
            pdev_ref[:, at] = high_low(jnp.exp(cum[:, at] + before))
            before = before + last
            rows.append(jnp.sum(jnp.where(mask, jnp.exp(last), 0.0), 0, keepdims=True))
        sub = lax.broadcasted_iota(jnp.int32, (8, width), 0)
        table = jnp.zeros((8, width), F32)
        for block in range(blocks):
            table = jnp.where(sub == block, rows[block], table)
        total_ref[...] = table
        whole[...] = jnp.zeros_like(whole)

    at = pl.ds(pl.multiple_of((step + 1) * SPAN, SPAN), SPAN)
    added = block_state(
        slab, halo_x_ref, halo_bc_ref, x_ref, bc_ref, cwx_ref, cwbc_ref, cbx_ref, cbbc_ref,
        w_ref[:, at], xc_ref, xw_ref, bcv_ref,
    )
    whole[...] = (whole[...] + added) * total_ref[pl.ds(step + 1, 1), :]

    @pl.when(step == pl.num_programs(0) - 1)
    def _():
        state_ref[...] = whole[...]


def second_kernel(
    x_ref, bc_ref, halo_ref, cwx_ref, cwbc_ref, cbx_ref, cbbc_ref, w_ref, total_ref, state_ref,
    xc_in, xw_in, bcv_in,
    xc_ref, xw_ref, bcv_ref, message_ref,
    slab,
):
    width = x_ref.shape[1]
    half = width // 2
    added = block_state(
        slab, halo_ref.at[:, 0:width], halo_ref.at[:, width : width + 2 * STATE],
        x_ref, bc_ref, cwx_ref, cwbc_ref, cbx_ref, cbbc_ref,
        w_ref[...], xc_ref, xw_ref, bcv_ref,
    )
    table = total_ref[...]
    later = table[1:2, :] * table[2:3, :] * table[3:4, :]
    first = table[0:1, :]
    everything = state_ref[...] + added * (first * later)
    decay = first * later
    high = decay.astype(BF16).astype(F32)
    low = decay - high
    sub = lax.broadcasted_iota(jnp.int32, (16, 128), 0)
    extra = jnp.zeros((16, 128), F32)
    for side in range(2):
        for tile in range(4):
            at = slice(side * half + tile * 128, side * half + tile * 128 + 128)
            extra = jnp.where(sub == side * 8 + tile, high[:, at], extra)
            extra = jnp.where(sub == side * 8 + 4 + tile, low[:, at], extra)
    extra = extra.astype(BF16)
    for group in range(STATE // 8):
        rows = everything[group * 8 : group * 8 + 8, :]
        both = jnp.concatenate([rows[:, 0:half], rows[:, half:width]], 0)
        message_ref[group * 16 : group * 16 + 16, 0:half] = both.astype(BF16)
        message_ref[group * 16 : group * 16 + 16, half : half + 128] = extra


def prefix_kernel(message_ref, out_ref):
    rows, width = out_ref.shape

    def decay_of(extra):
        return jnp.concatenate(
            [
                jnp.broadcast_to(extra[q : q + 1, :] + extra[q + 4 : q + 5, :], (8, 128))
                for q in range(width // 128)
            ],
            1,
        )

    carried = jnp.zeros((8, width), F32)
    for pair in range(rows // 16):
        at = slice(pair * 16, pair * 16 + 16)
        both = message_ref[at, :].astype(F32)
        middle = decay_of(both[0:8, width:]) * carried + both[0:8, 0:width]
        out_ref[at, :] = jnp.concatenate([carried, middle], 0).astype(BF16)
        carried = decay_of(both[8:16, width:]) * middle + both[8:16, 0:width]


def middle_kernel(xw_ref, xc_ref, bcv_ref, p_ref, total_ref, skip_ref, y_ref, state):
    step = pl.program_id(0)
    width = xw_ref.shape[1]
    heads = width // HEAD_DIM

    @pl.when(step == 0)
    def _():
        state[...] = jnp.zeros_like(state)

    b_part = bcv_ref[:, 0:STATE]
    c_part = bcv_ref[:, STATE : 2 * STATE]
    scores = lax.dot_general(
        c_part, b_part, (((1,), (1,)), ((), ())), preferred_element_type=F32
    )
    row = lax.broadcasted_iota(jnp.int32, (SPAN, SPAN), 0)
    lane = lax.broadcasted_iota(jnp.int32, (SPAN, SPAN), 1)
    masked = jnp.where(row >= lane, scores, 0.0).astype(BF16)
    weighted = xw_ref[...]
    total = jnp.dot(masked, weighted, preferred_element_type=F32) + jnp.dot(
        c_part, state[...].astype(BF16), preferred_element_type=F32
    )
    head_row = lax.broadcasted_iota(jnp.int32, (1, width), 1) // HEAD_DIM
    skip = jnp.zeros((1, width), F32)
    for head in range(heads):
        skip = jnp.where(head_row == head, skip_ref[head], skip)
    grown = spread(p_ref[...], expander(heads, width))
    y_ref[...] = grown * total + skip * xc_ref[...].astype(F32)
    added = lax.dot_general(
        b_part, weighted, (((0,), (0,)), ((), ())), preferred_element_type=F32
    )
    state[...] = (state[...] + added) * total_ref[pl.ds(step, 1), :]


def gate_kernel(start_ref, c_ref, p_ref, y_ref, z_ref, gated_ref, sum_ref, start):
    width = y_ref.shape[1]
    heads = width // HEAD_DIM
    half = width // 2

    @pl.when(pl.program_id(0) == 0)
    def _():
        for pair in range(STATE // 16):
            block = start_ref[pair * 32 : pair * 32 + 32, :].astype(F32)
            for side in range(2):
                rows = jnp.concatenate(
                    [block[side * 8 : side * 8 + 8, :], block[16 + side * 8 : 24 + side * 8, :]], 0
                )
                start[pair * 16 : pair * 16 + 16, side * half : side * half + half] = rows.astype(
                    BF16
                )

    product = jnp.dot(c_ref[...], start[...], preferred_element_type=F32)
    grown = spread(p_ref[...], expander(heads, width))
    squares = jnp.zeros((SPAN, 128), F32)
    for tile in range(width // 128):
        at = slice(tile * 128, tile * 128 + 128)
        gated = (y_ref[:, at] + grown[:, at] * product[:, at]) * half_silu(
            z_ref[:, at].astype(F32) * 0.5
        )
        gated_ref[:, at] = gated
        squares = squares + gated * gated
    for piece in range(SPAN // 128):
        at = slice(piece * 128, piece * 128 + 128)
        line = jnp.sum(jnp.transpose(squares[at, :]), 0, keepdims=True)
        sum_ref[:, at] = jnp.broadcast_to(line, (sum_ref.shape[0], 128))


def scale_kernel(gated_ref, sum_ref, gain_ref, out_ref):
    width = gated_ref.shape[1]
    total = jnp.sum(sum_ref[...], 0, keepdims=True)
    factor = lax.rsqrt(total / DI + EPSILON)
    for piece in range(SPAN // 128):
        rows = slice(piece * 128, piece * 128 + 128)
        column = jnp.transpose(jnp.broadcast_to(factor[:, rows], (128, 128)))
        for tile in range(width // 128):
            at = slice(tile * 128, tile * 128 + 128)
            out_ref[rows, at] = (gated_ref[rows, at] * column * gain_ref[:, at]).astype(BF16)


def whole_block(shape):
    return pl.BlockSpec(shape, lambda *_: (0,) * len(shape))


def params(grid=True, limit=24):
    return pltpu.CompilerParams(
        dimension_semantics=("arbitrary",) if grid else None, vmem_limit_bytes=limit << 20
    )


def cost(flops, moved):
    return pl.CostEstimate(flops=flops, bytes_accessed=moved, transcendentals=0)


SMEM = pl.BlockSpec(memory_space=pltpu.SMEM)


def local(
    x_input, bc_input, z_gate, dt_input, conv_weight_x, conv_weight_bc, conv_bias_x, conv_bias_bc,
    dt_bias, decay_log, skip_scale, norm_gain,
):
    tokens, width = x_input.shape
    heads = dt_input.shape[0]
    blocks = tokens // SPAN
    seq = lax.axis_size("seq")
    tp = lax.axis_size("tp")
    bcw = bc_input.shape[1]
    half = width // 2
    tail = jnp.concatenate([x_input[-8:], bc_input[-8:]], 1)
    halo = lax.ppermute(tail, "seq", [(k, k + 1) for k in range(seq - 1)])
    cbx = conv_bias_x.reshape(1, width)
    cbbc = conv_bias_bc.reshape(1, bcw)
    gain = norm_gain.reshape(1, width)

    def rows_of(columns, ahead=0):
        return pl.BlockSpec((SPAN, columns), lambda k: (k + ahead, 0))

    def halo_of(columns):
        return pl.BlockSpec((8, columns), lambda k: ((k + 1) * (SPAN // 8) - 1, 0))

    def lanes_of(count):
        return pl.BlockSpec((count, SPAN), lambda k: (0, k))

    weights = [whole_block((4, width)), whole_block((4, bcw)), whole_block((1, width)), whole_block((1, bcw))]
    slab = pltpu.VMEM((width // 128 + 2, SPAN + 8, 128), F32)
    pair = jax.ShapeDtypeStruct((2 * heads, tokens), BF16)
    xc, xw, bcv, w, p, pdev, total, state = pl.pallas_call(
        first_kernel,
        grid=(blocks - 1,),
        in_specs=[
            rows_of(width, 1), halo_of(width), rows_of(bcw, 1), halo_of(bcw),
            whole_block((heads, tokens)), *weights, SMEM, SMEM,
        ],
        out_specs=[
            rows_of(width, 1), rows_of(width, 1), rows_of(bcw, 1),
            whole_block(pair.shape), whole_block(pair.shape), whole_block(pair.shape),
            whole_block((8, width)), whole_block((STATE, width)),
        ],
        out_shape=[
            jax.ShapeDtypeStruct((tokens, width), BF16),
            jax.ShapeDtypeStruct((tokens, width), BF16),
            jax.ShapeDtypeStruct((tokens, bcw), BF16),
            pair, pair, pair,
            jax.ShapeDtypeStruct((8, width), F32),
            jax.ShapeDtypeStruct((STATE, width), F32),
        ],
        scratch_shapes=[slab, pltpu.VMEM((STATE, width), F32)],
        compiler_params=params(),
        cost_estimate=cost(20_000_000_000, 10 << 20),
        name="first",
    )(
        x_input, x_input, bc_input, bc_input, dt_input, conv_weight_x, conv_weight_bc, cbx, cbbc,
        dt_bias, decay_log,
    )

    anywhere = pl.BlockSpec(memory_space=pl.ANY)
    xc, xw, bcv, message = pl.pallas_call(
        second_kernel,
        grid=(1,),
        in_specs=[
            rows_of(width), rows_of(bcw), whole_block((8, width + bcw)), *weights,
            lanes_of(2 * heads), whole_block((8, width)), whole_block((STATE, width)),
            anywhere, anywhere, anywhere,
        ],
        out_specs=[
            rows_of(width), rows_of(width), rows_of(bcw), whole_block((2 * STATE, half + 128)),
        ],
        out_shape=[
            jax.ShapeDtypeStruct((tokens, width), BF16),
            jax.ShapeDtypeStruct((tokens, width), BF16),
            jax.ShapeDtypeStruct((tokens, bcw), BF16),
            jax.ShapeDtypeStruct((2 * STATE, half + 128), BF16),
        ],
        scratch_shapes=[slab],
        input_output_aliases={10: 0, 11: 1, 12: 2},
        compiler_params=params(),
        cost_estimate=cost(5_000_000_000, 4 << 20),
        name="second",
    )(
        x_input, bc_input, halo, conv_weight_x, conv_weight_bc, cbx, cbbc, w, total, state,
        xc, xw, bcv,
    )

    sent = lax.all_to_all(message, "seq", 0, 0, tiled=True)

    y = pl.pallas_call(
        middle_kernel,
        grid=(blocks,),
        in_specs=[
            rows_of(width), rows_of(width), rows_of(bcw), lanes_of(2 * heads),
            whole_block((8, width)), SMEM,
        ],
        out_specs=rows_of(width),
        out_shape=jax.ShapeDtypeStruct((tokens, width), F32),
        scratch_shapes=[pltpu.VMEM((STATE, width), F32)],
        compiler_params=params(),
        cost_estimate=cost(20_000_000_000, 10 << 20),
        name="middle",
    )(xw, xc, bcv, p, total, skip_scale)

    starts = pl.pallas_call(
        prefix_kernel,
        out_shape=jax.ShapeDtypeStruct((2 * STATE, half), BF16),
        compiler_params=params(False),
        cost_estimate=cost(2_000_000_000, 1 << 20),
        name="prefix",
    )(sent)
    mine = lax.all_to_all(starts, "seq", 0, 0, tiled=True)

    gated, sums = pl.pallas_call(
        gate_kernel,
        grid=(blocks,),
        in_specs=[
            whole_block((2 * STATE, half)),
            pl.BlockSpec((SPAN, STATE), lambda k: (k, 1)),
            lanes_of(2 * heads), rows_of(width), rows_of(width),
        ],
        out_specs=[rows_of(width), lanes_of(tp)],
        out_shape=[
            jax.ShapeDtypeStruct((tokens, width), F32), jax.ShapeDtypeStruct((tp, tokens), F32)
        ],
        scratch_shapes=[pltpu.VMEM((STATE, width), BF16)],
        compiler_params=params(),
        cost_estimate=cost(10_000_000_000, 10 << 20),
        name="gate",
    )(mine, bcv, pdev, y, z_gate)

    all_sums = lax.all_to_all(sums, "tp", 0, 0, tiled=True)

    return pl.pallas_call(
        scale_kernel,
        grid=(blocks,),
        in_specs=[rows_of(width), lanes_of(tp), whole_block((1, width))],
        out_specs=rows_of(width),
        out_shape=jax.ShapeDtypeStruct((tokens, width), BF16),
        compiler_params=params(),
        cost_estimate=cost(5_000_000_000, 6 << 20),
        name="scale",
    )(gated, all_sums, gain)


def solution(mesh):
    return jax.shard_map(
        local,
        mesh=mesh,
        in_specs=(
            P("seq", "tp"), P("seq", "tp"), P("seq", "tp"), P("tp", "seq"),
            P(None, "tp"), P(None, "tp"),
            P("tp"), P("tp"), P("tp"), P("tp"), P("tp"), P("tp"),
        ),
        out_specs=P("seq", "tp"),
        check_vma=False,
    )
```

```python
import functools

import jax
import jax.numpy as jnp
from jax import lax
from jax.experimental import pallas as pl
from jax.experimental.pallas import tpu as pltpu
from jax.sharding import PartitionSpec as P

HEAD_DIM = 64
STATE = 128
SPAN = 256
DI = 8192
EPSILON = 1e-05

F32 = jnp.float32
BF16 = jnp.bfloat16


def column_of(scalars, count):
    rows = lax.broadcasted_iota(jnp.int32, (count, 128), 0)
    column = jnp.zeros((count, 128), F32)
    for head in range(count):
        column = jnp.where(rows == head, scalars[head], column)
    return column


def head_mask(heads, width):
    row = lax.broadcasted_iota(jnp.int32, (heads, width), 0)
    lane = lax.broadcasted_iota(jnp.int32, (heads, width), 1)
    return lane // HEAD_DIM == row


def expander(heads, width):
    one_hot = jnp.where(head_mask(heads, width), 1.0, 0.0)
    return jnp.concatenate([one_hot, one_hot], 0).astype(BF16)


def high_low(value):
    high = value.astype(BF16).astype(F32)
    return jnp.concatenate([high, value - high], 0).astype(BF16)


def spread(pair, one_hot):
    return lax.dot_general(pair, one_hot, (((0,), (0,)), ((), ())), preferred_element_type=F32)


def half_silu(half):
    return half + half * jnp.tanh(half)


def conv_tile(slab, tile, x_tile, halo_tile, weight, bias):
    rows = x_tile.shape[0]
    slab[tile, 0:8, :] = halo_tile.astype(F32)
    slab[tile, 8 : 8 + rows, :] = x_tile.astype(F32)
    total = bias
    for tap in range(4):
        total = total + slab[tile, 5 + tap : 5 + tap + rows, :] * weight[tap : tap + 1, :]
    return half_silu(total).astype(BF16)


def block_state(slab, halo_x, halo_bc, x, bc, cwx, cwbc, cbx, cbbc, pair, xc_out, xw_out, bc_out):
    width = x.shape[1]
    heads = width // HEAD_DIM
    tiles = width // 128
    for tile in range(2):
        at = slice(tile * 128, tile * 128 + 128)
        bc_out[:, at] = conv_tile(
            slab,
            tiles + tile,
            bc[:, at],
            halo_bc[:, at],
            cwbc[:, at].astype(F32) * 0.5,
            cbbc[:, at] * 0.5,
        )
    weight = spread(pair, expander(heads, width))
    for tile in range(tiles):
        at = slice(tile * 128, tile * 128 + 128)
        conv = conv_tile(
            slab, tile, x[:, at], halo_x[:, at], cwx[:, at].astype(F32) * 0.5, cbx[:, at] * 0.5
        )
        xc_out[:, at] = conv
        xw_out[:, at] = (conv.astype(F32) * weight[:, at]).astype(BF16)
    return lax.dot_general(
        bc_out[:, 0:STATE], xw_out[...], (((0,), (0,)), ((), ())), preferred_element_type=F32
    )


def first_kernel(
    x_ref, halo_x_ref, bc_ref, halo_bc_ref, dt_ref, cwx_ref, cwbc_ref, cbx_ref, cbbc_ref,
    dt_bias_ref, decay_ref,
    xc_ref, xw_ref, bcv_ref, w_ref, p_ref, pdev_ref, total_ref, state_ref,
    slab, whole,
):
    step = pl.program_id(0)
    heads, tokens = dt_ref.shape
    width = x_ref.shape[1]
    blocks = tokens // SPAN

    @pl.when(step == 0)
    def _():
        repeat = tokens // 128
        bias = jnp.concatenate([column_of(dt_bias_ref, heads)] * repeat, 1)
        rate = jnp.concatenate([jnp.exp(column_of(decay_ref, heads))] * repeat, 1)
        raw = dt_ref[...].astype(F32) + bias
        size = jnp.maximum(raw, 0.0) + jnp.log(1.0 + jnp.exp(-jnp.abs(raw)))
        cum = -rate * size
        position = lax.broadcasted_iota(jnp.int32, (heads, tokens), 1) & (SPAN - 1)
        shift = 1
        while shift < SPAN:
            cum = cum + jnp.where(position >= shift, pltpu.roll(cum, shift, 1), 0.0)
            shift *= 2
        w_ref[...] = high_low(jnp.exp(-cum) * size)
        p_ref[...] = high_low(jnp.exp(cum))
        mask = head_mask(heads, width)
        before = jnp.zeros((heads, 1), F32)
        rows = []
        for block in range(blocks):
            at = slice(block * SPAN, block * SPAN + SPAN)
            last = cum[:, block * SPAN + SPAN - 1 : block * SPAN + SPAN]
            pdev_ref[:, at] = high_low(jnp.exp(cum[:, at] + before))
            before = before + last
            rows.append(jnp.sum(jnp.where(mask, jnp.exp(last), 0.0), 0, keepdims=True))
        sub = lax.broadcasted_iota(jnp.int32, (8, width), 0)
        table = jnp.zeros((8, width), F32)
        for block in range(blocks):
            table = jnp.where(sub == block, rows[block], table)
        total_ref[...] = table
        whole[...] = jnp.zeros_like(whole)

    at = pl.ds(pl.multiple_of((step + 1) * SPAN, SPAN), SPAN)
    added = block_state(
        slab, halo_x_ref, halo_bc_ref, x_ref, bc_ref, cwx_ref, cwbc_ref, cbx_ref, cbbc_ref,
        w_ref[:, at], xc_ref.at[at, :], xw_ref.at[at, :], bcv_ref.at[at, :],
    )
    whole[...] = (whole[...] + added) * total_ref[pl.ds(step + 1, 1), :]

    @pl.when(step == pl.num_programs(0) - 1)
    def _():
        state_ref[...] = whole[...]


def second_kernel(
    x_ref, bc_ref, halo_ref, cwx_ref, cwbc_ref, cbx_ref, cbbc_ref, w_ref, total_ref, state_ref,
    xc_in, xw_in, bcv_in,
    xc_ref, xw_ref, bcv_ref, message_ref,
    slab,
):
    width = x_ref.shape[1]
    half = width // 2
    at = slice(0, SPAN)
    added = block_state(
        slab, halo_ref.at[:, 0:width], halo_ref.at[:, width : width + 2 * STATE],
        x_ref, bc_ref, cwx_ref, cwbc_ref, cbx_ref, cbbc_ref,
        w_ref[:, at], xc_ref.at[at, :], xw_ref.at[at, :], bcv_ref.at[at, :],
    )
    table = total_ref[...]
    later = table[1:2, :] * table[2:3, :] * table[3:4, :]
    first = table[0:1, :]
    everything = state_ref[...] + added * (first * later)
    decay = first * later
    high = decay.astype(BF16).astype(F32)
    low = decay - high
    sub = lax.broadcasted_iota(jnp.int32, (16, 128), 0)
    extra = jnp.zeros((16, 128), F32)
    for side in range(2):
        for tile in range(4):
            at = slice(side * half + tile * 128, side * half + tile * 128 + 128)
            extra = jnp.where(sub == side * 8 + tile, high[:, at], extra)
            extra = jnp.where(sub == side * 8 + 4 + tile, low[:, at], extra)
    extra = extra.astype(BF16)
    for group in range(STATE // 8):
        rows = everything[group * 8 : group * 8 + 8, :]
        both = jnp.concatenate([rows[:, 0:half], rows[:, half:width]], 0)
        message_ref[group * 16 : group * 16 + 16, 0:half] = both.astype(BF16)
        message_ref[group * 16 : group * 16 + 16, half : half + 128] = extra


def prefix_kernel(message_ref, out_ref):
    rows, width = out_ref.shape

    def decay_of(extra):
        return jnp.concatenate(
            [
                jnp.broadcast_to(extra[q : q + 1, :] + extra[q + 4 : q + 5, :], (8, 128))
                for q in range(width // 128)
            ],
            1,
        )

    carried = jnp.zeros((8, width), F32)
    for pair in range(rows // 16):
        at = slice(pair * 16, pair * 16 + 16)
        both = message_ref[at, :].astype(F32)
        middle = decay_of(both[0:8, width:]) * carried + both[0:8, 0:width]
        out_ref[at, :] = jnp.concatenate([carried, middle], 0).astype(BF16)
        carried = decay_of(both[8:16, width:]) * middle + both[8:16, 0:width]


def tail_kernel(x_ref, bc_ref, out_ref):
    width = x_ref.shape[1]
    out_ref[:, 0:width] = x_ref[...]
    out_ref[:, width:] = bc_ref[...]


def middle_kernel(xw_ref, xc_ref, bcv_ref, p_ref, total_ref, skip_ref, y_ref, state):
    step = pl.program_id(0)
    width = xw_ref.shape[1]
    heads = width // HEAD_DIM

    @pl.when(step == 0)
    def _():
        state[...] = jnp.zeros_like(state)

    b_part = bcv_ref[:, 0:STATE]
    c_part = bcv_ref[:, STATE : 2 * STATE]
    scores = lax.dot_general(
        c_part, b_part, (((1,), (1,)), ((), ())), preferred_element_type=F32
    )
    row = lax.broadcasted_iota(jnp.int32, (SPAN, SPAN), 0)
    lane = lax.broadcasted_iota(jnp.int32, (SPAN, SPAN), 1)
    masked = jnp.where(row >= lane, scores, 0.0).astype(BF16)
    weighted = xw_ref[...]
    total = jnp.dot(masked, weighted, preferred_element_type=F32) + jnp.dot(
        c_part, state[...].astype(BF16), preferred_element_type=F32
    )
    head_row = lax.broadcasted_iota(jnp.int32, (1, width), 1) // HEAD_DIM
    skip = jnp.zeros((1, width), F32)
    for head in range(heads):
        skip = jnp.where(head_row == head, skip_ref[head], skip)
    grown = spread(p_ref[...], expander(heads, width))
    y_ref[...] = grown * total + skip * xc_ref[...].astype(F32)
    added = lax.dot_general(
        b_part, weighted, (((0,), (0,)), ((), ())), preferred_element_type=F32
    )
    state[...] = (state[...] + added) * total_ref[pl.ds(step, 1), :]


def gate_kernel(start_ref, c_ref, p_ref, y_ref, z_ref, gated_ref, sum_ref, start):
    width = y_ref.shape[1]
    heads = width // HEAD_DIM
    half = width // 2

    @pl.when(pl.program_id(0) == 0)
    def _():
        for pair in range(STATE // 16):
            block = start_ref[pair * 32 : pair * 32 + 32, :].astype(F32)
            for side in range(2):
                rows = jnp.concatenate(
                    [block[side * 8 : side * 8 + 8, :], block[16 + side * 8 : 24 + side * 8, :]], 0
                )
                start[pair * 16 : pair * 16 + 16, side * half : side * half + half] = rows.astype(
                    BF16
                )

    product = jnp.dot(c_ref[...], start[...], preferred_element_type=F32)
    grown = spread(p_ref[...], expander(heads, width))
    squares = jnp.zeros((SPAN, 128), F32)
    for tile in range(width // 128):
        at = slice(tile * 128, tile * 128 + 128)
        gated = (y_ref[:, at] + grown[:, at] * product[:, at]) * half_silu(
            z_ref[:, at].astype(F32) * 0.5
        )
        gated_ref[:, at] = gated
        squares = squares + gated * gated
    for piece in range(SPAN // 128):
        at = slice(piece * 128, piece * 128 + 128)
        line = jnp.sum(jnp.transpose(squares[at, :]), 0, keepdims=True)
        sum_ref[:, at] = jnp.broadcast_to(line, (sum_ref.shape[0], 128))


def scale_kernel(gated_ref, sum_ref, gain_ref, out_ref):
    width = gated_ref.shape[1]
    total = jnp.sum(sum_ref[...], 0, keepdims=True)
    factor = lax.rsqrt(total / DI + EPSILON)
    for piece in range(gated_ref.shape[0] // 128):
        rows = slice(piece * 128, piece * 128 + 128)
        column = jnp.transpose(jnp.broadcast_to(factor[:, rows], (128, 128)))
        for tile in range(width // 128):
            at = slice(tile * 128, tile * 128 + 128)
            out_ref[rows, at] = (gated_ref[rows, at] * column * gain_ref[:, at]).astype(BF16)


def whole_block(shape):
    return pl.BlockSpec(shape, lambda *_: (0,) * len(shape))


def params(grid=True, limit=24):
    return pltpu.CompilerParams(
        dimension_semantics=("arbitrary",) if grid else None, vmem_limit_bytes=limit << 20
    )


def cost(flops, moved):
    return pl.CostEstimate(flops=flops, bytes_accessed=moved, transcendentals=0)


SMEM = pl.BlockSpec(memory_space=pltpu.SMEM)
VMEM = pl.BlockSpec(memory_space=pltpu.VMEM)


def in_hbm(array):
    return pltpu.with_memory_space_constraint(array, pltpu.HBM)


def local(
    x_input, bc_input, z_gate, dt_input, conv_weight_x, conv_weight_bc, conv_bias_x, conv_bias_bc,
    dt_bias, decay_log, skip_scale, norm_gain,
):
    tokens, width = x_input.shape
    heads = dt_input.shape[0]
    blocks = tokens // SPAN
    seq = lax.axis_size("seq")
    tp = lax.axis_size("tp")
    bcw = bc_input.shape[1]
    half = width // 2
    last = tokens // 8 - 1
    tail = pl.pallas_call(
        tail_kernel,
        grid=(1,),
        in_specs=[
            pl.BlockSpec((8, width), lambda k: (last, 0)), pl.BlockSpec((8, bcw), lambda k: (last, 0))
        ],
        out_specs=VMEM,
        out_shape=pltpu.VMEM((8, width + bcw), BF16),
        compiler_params=params(limit=4),
        name="tail",
    )(in_hbm(x_input), in_hbm(bc_input))
    halo = lax.ppermute(tail, "seq", [(k, k + 1) for k in range(seq - 1)])
    cbx = conv_bias_x.reshape(1, width)
    cbbc = conv_bias_bc.reshape(1, bcw)
    gain = norm_gain.reshape(1, width)

    def rows_of(columns, ahead=0):
        return pl.BlockSpec((SPAN, columns), lambda k: (k + ahead, 0))

    def halo_of(columns):
        return pl.BlockSpec((8, columns), lambda k: ((k + 1) * (SPAN // 8) - 1, 0))

    def lanes_of(count):
        return pl.BlockSpec((count, SPAN), lambda k: (0, k))

    weights = [whole_block((4, width)), whole_block((4, bcw)), whole_block((1, width)), whole_block((1, bcw))]
    slab = pltpu.VMEM((width // 128 + 2, SPAN + 8, 128), F32)
    pair = pltpu.VMEM((2 * heads, tokens), BF16)
    wide = pltpu.VMEM((tokens, width), BF16)
    float_wide = pltpu.VMEM((tokens, width), F32)
    narrow = pltpu.VMEM((tokens, bcw), BF16)
    xc, xw, bcv, w, p, pdev, total, state = pl.pallas_call(
        first_kernel,
        grid=(blocks - 1,),
        in_specs=[
            rows_of(width, 1), halo_of(width), rows_of(bcw, 1), halo_of(bcw),
            whole_block((heads, tokens)), *weights, SMEM, SMEM,
        ],
        out_specs=[VMEM] * 8,
        out_shape=[
            wide, wide, narrow, pair, pair, pair,
            pltpu.VMEM((8, width), F32), pltpu.VMEM((STATE, width), F32),
        ],
        scratch_shapes=[slab, pltpu.VMEM((STATE, width), F32)],
        compiler_params=params(limit=16),
        cost_estimate=cost(20_000_000_000, 10 << 20),
        name="first",
    )(
        in_hbm(x_input), in_hbm(x_input), in_hbm(bc_input), in_hbm(bc_input), in_hbm(dt_input),
        in_hbm(conv_weight_x), in_hbm(conv_weight_bc), in_hbm(cbx), in_hbm(cbbc),
        dt_bias, decay_log,
    )

    xc, xw, bcv, message = pl.pallas_call(
        second_kernel,
        grid=(1,),
        in_specs=[
            rows_of(width), rows_of(bcw), VMEM, *weights, VMEM, VMEM, VMEM, VMEM, VMEM, VMEM,
        ],
        out_specs=[VMEM] * 4,
        out_shape=[wide, wide, narrow, pltpu.VMEM((2 * STATE, half + 128), BF16)],
        scratch_shapes=[slab],
        input_output_aliases={10: 0, 11: 1, 12: 2},
        compiler_params=params(limit=16),
        cost_estimate=cost(5_000_000_000, 4 << 20),
        name="second",
    )(
        x_input, bc_input, halo, conv_weight_x, conv_weight_bc, cbx, cbbc, w, total, state,
        xc, xw, bcv,
    )

    sent = lax.all_to_all(message, "seq", 0, 0, tiled=True)

    y = pl.pallas_call(
        middle_kernel,
        grid=(blocks,),
        in_specs=[
            rows_of(width), rows_of(width), rows_of(bcw), lanes_of(2 * heads),
            whole_block((8, width)), SMEM,
        ],
        out_specs=rows_of(width),
        out_shape=pltpu.HBM((tokens, width), F32),
        scratch_shapes=[pltpu.VMEM((STATE, width), F32)],
        compiler_params=params(limit=16),
        cost_estimate=cost(20_000_000_000, 10 << 20),
        name="middle",
    )(in_hbm(xw), in_hbm(xc), bcv, p, total, skip_scale)

    starts = pl.pallas_call(
        prefix_kernel,
        in_specs=[VMEM],
        out_specs=VMEM,
        out_shape=pltpu.VMEM((2 * STATE, half), BF16),
        compiler_params=params(False, 4),
        cost_estimate=cost(2_000_000_000, 1 << 20),
        name="prefix",
    )(sent)
    mine = lax.all_to_all(starts, "seq", 0, 0, tiled=True)

    gated, sums = pl.pallas_call(
        gate_kernel,
        grid=(blocks,),
        in_specs=[
            whole_block((2 * STATE, half)),
            pl.BlockSpec((SPAN, STATE), lambda k: (k, 1)),
            lanes_of(2 * heads), rows_of(width), rows_of(width),
        ],
        out_specs=[rows_of(width), lanes_of(tp)],
        out_shape=[
            jax.ShapeDtypeStruct((tokens, width), F32), jax.ShapeDtypeStruct((tp, tokens), F32)
        ],
        scratch_shapes=[pltpu.VMEM((STATE, width), BF16)],
        compiler_params=params(limit=24),
        cost_estimate=cost(10_000_000_000, 10 << 20),
        name="gate",
    )(mine, bcv, pdev, in_hbm(y), z_gate)

    all_sums = lax.all_to_all(sums, "tp", 0, 0, tiled=True)

    return pl.pallas_call(
        scale_kernel,
        grid=(blocks,),
        in_specs=[rows_of(width), lanes_of(tp), whole_block((1, width))],
        out_specs=rows_of(width),
        out_shape=jax.ShapeDtypeStruct((tokens, width), BF16),
        compiler_params=params(),
        cost_estimate=cost(5_000_000_000, 6 << 20),
        name="scale",
    )(gated, all_sums, gain)


def solution(mesh):
    return jax.shard_map(
        local,
        mesh=mesh,
        in_specs=(
            P("seq", "tp"), P("seq", "tp"), P("seq", "tp"), P("tp", "seq"),
            P(None, "tp"), P(None, "tp"),
            P("tp"), P("tp"), P("tp"), P("tp"), P("tp"), P("tp"),
        ),
        out_specs=P("seq", "tp"),
        check_vma=False,
    )
```

```python
import functools

import jax
import jax.numpy as jnp
from jax import lax
from jax.experimental import pallas as pl
from jax.experimental.pallas import tpu as pltpu
from jax.sharding import PartitionSpec as P

HEAD_DIM = 64
STATE = 128
SPAN = 256
DI = 8192
EPSILON = 1e-05

F32 = jnp.float32
BF16 = jnp.bfloat16


def column_of(line):
    count = line.shape[1]
    row = lax.broadcasted_iota(jnp.int32, (count, count), 0)
    lane = lax.broadcasted_iota(jnp.int32, (count, count), 1)
    return jnp.sum(jnp.where(row == lane, line, 0.0), 1, keepdims=True)


def head_mask(heads, width):
    row = lax.broadcasted_iota(jnp.int32, (heads, width), 0)
    lane = lax.broadcasted_iota(jnp.int32, (heads, width), 1)
    return lane // HEAD_DIM == row


def expander(heads, width):
    one_hot = jnp.where(head_mask(heads, width), 1.0, 0.0)
    return jnp.concatenate([one_hot, one_hot], 0).astype(BF16)


def high_low(value):
    high = value.astype(BF16).astype(F32)
    return jnp.concatenate([high, value - high], 0).astype(BF16)


def spread(pair, one_hot):
    return lax.dot_general(pair, one_hot, (((0,), (0,)), ((), ())), preferred_element_type=F32)


def half_silu(half):
    return half + half * jnp.tanh(half)


def conv_tile(slab, tile, x_tile, halo_tile, weight, bias):
    rows = x_tile.shape[0]
    slab[tile, 0:8, :] = halo_tile.astype(F32)
    slab[tile, 8 : 8 + rows, :] = x_tile.astype(F32)
    total = bias
    for tap in range(4):
        total = total + slab[tile, 5 + tap : 5 + tap + rows, :] * weight[tap : tap + 1, :]
    return half_silu(total).astype(BF16)


def block_state(slab, xw, halo_x, halo_bc, x, bc, cwx, cwbc, cbx, cbbc, pair, xc_out, bc_out):
    width = x.shape[1]
    heads = width // HEAD_DIM
    tiles = width // 128
    for tile in range(2):
        at = slice(tile * 128, tile * 128 + 128)
        bc_out[:, at] = conv_tile(
            slab,
            tiles + tile,
            bc[:, at],
            halo_bc[:, at],
            cwbc[:, at].astype(F32) * 0.5,
            cbbc[:, at] * 0.5,
        )
    weight = spread(pair, expander(heads, width))
    for tile in range(tiles):
        at = slice(tile * 128, tile * 128 + 128)
        conv = conv_tile(
            slab, tile, x[:, at], halo_x[:, at], cwx[:, at].astype(F32) * 0.5, cbx[:, at] * 0.5
        )
        xc_out[:, at] = conv
        xw[:, at] = (conv.astype(F32) * weight[:, at]).astype(BF16)
    return lax.dot_general(
        bc_out[:, 0:STATE], xw[...], (((0,), (0,)), ((), ())), preferred_element_type=F32
    )


def first_kernel(
    x_ref, halo_x_ref, bc_ref, halo_bc_ref, tail_x_ref, tail_bc_ref, dt_ref,
    cwx_ref, cwbc_ref, cbx_ref, cbbc_ref, dt_bias_ref, decay_ref,
    tail_ref, xc_ref, bcv_ref, w_ref, p_ref, pdev_ref, total_ref, state_ref,
    slab, xw,
):
    heads, tokens = dt_ref.shape
    width = x_ref.shape[1]
    blocks = tokens // SPAN
    tail_ref[:, 0:width] = tail_x_ref[...]
    tail_ref[:, width:] = tail_bc_ref[...]
    rate = jnp.exp(column_of(decay_ref[...]))
    raw = dt_ref[...].astype(F32) + column_of(dt_bias_ref[...])
    size = jnp.maximum(raw, 0.0) + jnp.log(1.0 + jnp.exp(-jnp.abs(raw)))
    cum = -rate * size
    position = lax.broadcasted_iota(jnp.int32, (heads, tokens), 1) & (SPAN - 1)
    shift = 1
    while shift < SPAN:
        cum = cum + jnp.where(position >= shift, pltpu.roll(cum, shift, 1), 0.0)
        shift *= 2
    w_ref[...] = high_low(jnp.exp(-cum) * size)
    p_ref[...] = high_low(jnp.exp(cum))
    mask = head_mask(heads, width)
    before = jnp.zeros((heads, 1), F32)
    sub = lax.broadcasted_iota(jnp.int32, (8, width), 0)
    table = jnp.zeros((8, width), F32)
    for block in range(blocks):
        at = slice(block * SPAN, block * SPAN + SPAN)
        last = cum[:, block * SPAN + SPAN - 1 : block * SPAN + SPAN]
        pdev_ref[:, at] = high_low(jnp.exp(cum[:, at] + before))
        before = before + last
        row = jnp.sum(jnp.where(mask, jnp.exp(last), 0.0), 0, keepdims=True)
        table = jnp.where(sub == block, row, table)
    total_ref[...] = table
    added = block_state(
        slab, xw, halo_x_ref, halo_bc_ref, x_ref, bc_ref, cwx_ref, cwbc_ref, cbx_ref, cbbc_ref,
        w_ref[:, SPAN : 2 * SPAN], xc_ref.at[SPAN : 2 * SPAN, :], bcv_ref.at[SPAN : 2 * SPAN, :],
    )
    state_ref[...] = added * table[1:2, :]


def later_kernel(
    x_ref, bc_ref, cwx_ref, cwbc_ref, cbx_ref, cbbc_ref, w_ref, total_ref, state_in, xc_in, bcv_in,
    xc_ref, bcv_ref, state_ref,
    slab, xw,
):
    tokens = x_ref.shape[0]
    for block in range(2, tokens // SPAN):
        at = slice(block * SPAN, block * SPAN + SPAN)
        ahead = slice(block * SPAN - 8, block * SPAN)
        added = block_state(
            slab, xw, x_ref.at[ahead, :], bc_ref.at[ahead, :], x_ref.at[at, :], bc_ref.at[at, :],
            cwx_ref, cwbc_ref, cbx_ref, cbbc_ref,
            w_ref[:, at], xc_ref.at[at, :], bcv_ref.at[at, :],
        )
        previous = state_in if block == 2 else state_ref
        state_ref[...] = (previous[...] + added) * total_ref[block : block + 1, :]


def second_kernel(
    x_ref, bc_ref, halo_ref, cwx_ref, cwbc_ref, cbx_ref, cbbc_ref, w_ref, total_ref, state_ref,
    xc_in, bcv_in,
    xc_ref, bcv_ref, message_ref,
    slab, xw,
):
    width = x_ref.shape[1]
    half = width // 2
    at = slice(0, SPAN)
    added = block_state(
        slab, xw, halo_ref.at[:, 0:width], halo_ref.at[:, width : width + 2 * STATE],
        x_ref.at[at, :], bc_ref.at[at, :], cwx_ref, cwbc_ref, cbx_ref, cbbc_ref,
        w_ref[:, at], xc_ref.at[at, :], bcv_ref.at[at, :],
    )
    table = total_ref[...]
    decay = table[0:1, :] * (table[1:2, :] * table[2:3, :] * table[3:4, :])
    everything = state_ref[...] + added * decay
    high = decay.astype(BF16).astype(F32)
    low = decay - high
    sub = lax.broadcasted_iota(jnp.int32, (16, 128), 0)
    extra = jnp.zeros((16, 128), F32)
    for side in range(2):
        for tile in range(4):
            at = slice(side * half + tile * 128, side * half + tile * 128 + 128)
            extra = jnp.where(sub == side * 8 + tile, high[:, at], extra)
            extra = jnp.where(sub == side * 8 + 4 + tile, low[:, at], extra)
    extra = extra.astype(BF16)
    for group in range(STATE // 8):
        rows = everything[group * 8 : group * 8 + 8, :]
        both = jnp.concatenate([rows[:, 0:half], rows[:, half:width]], 0)
        message_ref[group * 16 : group * 16 + 16, 0:half] = both.astype(BF16)
        message_ref[group * 16 : group * 16 + 16, half : half + 128] = extra


def prefix_kernel(message_ref, after_ref, out_ref):
    rows, width = out_ref.shape

    def decay_of(extra):
        return jnp.concatenate(
            [
                jnp.broadcast_to(extra[q : q + 1, :] + extra[q + 4 : q + 5, :], (8, 128))
                for q in range(width // 128)
            ],
            1,
        )

    carried = jnp.zeros((8, width), F32)
    for pair in range(rows // 16):
        at = slice(pair * 16, pair * 16 + 16)
        both = message_ref[at, :].astype(F32)
        middle = decay_of(both[0:8, width:]) * carried + both[0:8, 0:width]
        out_ref[at, :] = jnp.concatenate([carried, middle], 0).astype(BF16)
        carried = decay_of(both[8:16, width:]) * middle + both[8:16, 0:width]


def middle_kernel(
    xc_ref, bcv_ref, w_ref, p_ref, total_ref, skip_ref, y_ref, state, xw, y, sem
):
    tokens, width = xc_ref.shape
    heads = width // HEAD_DIM
    head_row = lax.broadcasted_iota(jnp.int32, (1, width), 1) // HEAD_DIM
    skip = jnp.zeros((1, width), F32)
    for head in range(heads):
        skip = jnp.where(head_row == head, skip_ref[head], skip)
    one_hot = expander(heads, width)
    row = lax.broadcasted_iota(jnp.int32, (SPAN, SPAN), 0)
    lane = lax.broadcasted_iota(jnp.int32, (SPAN, SPAN), 1)
    copies = []
    for block in range(tokens // SPAN):
        at = slice(block * SPAN, block * SPAN + SPAN)
        b_part = bcv_ref[at, 0:STATE]
        c_part = bcv_ref[at, STATE : 2 * STATE]
        scores = lax.dot_general(
            c_part, b_part, (((1,), (1,)), ((), ())), preferred_element_type=F32
        )
        masked = jnp.where(row >= lane, scores, 0.0).astype(BF16)
        xw[...] = (xc_ref[at, :].astype(F32) * spread(w_ref[:, at], one_hot)).astype(BF16)
        total = jnp.dot(masked, xw[...], preferred_element_type=F32)
        if block > 0:
            total = total + jnp.dot(
                c_part, state[...].astype(BF16), preferred_element_type=F32
            )
        y[at, :] = spread(p_ref[:, at], one_hot) * total + skip * xc_ref[at, :].astype(F32)
        copy = pltpu.make_async_copy(y.at[at, :], y_ref.at[at, :], sem.at[block])
        copy.start()
        copies.append(copy)
        if (block + 1) * SPAN < tokens:
            added = lax.dot_general(
                b_part, xw[...], (((0,), (0,)), ((), ())), preferred_element_type=F32
            )
            if block > 0:
                added = added + state[...]
            state[...] = added * total_ref[block : block + 1, :]
    for copy in copies:
        copy.wait()


def gate_kernel(start_ref, bcv_ref, p_ref, y_ref, z_ref, gated_ref, sum_ref, start):
    tokens, width = y_ref.shape
    heads = width // HEAD_DIM
    half = width // 2
    for pair in range(STATE // 16):
        block = start_ref[pair * 32 : pair * 32 + 32, :].astype(F32)
        for side in range(2):
            rows = jnp.concatenate(
                [block[side * 8 : side * 8 + 8, :], block[16 + side * 8 : 24 + side * 8, :]], 0
            )
            start[pair * 16 : pair * 16 + 16, side * half : side * half + half] = rows.astype(BF16)
    one_hot = expander(heads, width)
    for block in range(tokens // SPAN):
        rows = slice(block * SPAN, block * SPAN + SPAN)
        product = jnp.dot(
            bcv_ref[rows, STATE : 2 * STATE], start[...], preferred_element_type=F32
        )
        grown = spread(p_ref[:, rows], one_hot)
        squares = jnp.zeros((SPAN, 128), F32)
        for tile in range(width // 128):
            at = slice(tile * 128, tile * 128 + 128)
            gated = (y_ref[rows, at] + grown[:, at] * product[:, at]) * half_silu(
                z_ref[rows, at].astype(F32) * 0.5
            )
            gated_ref[rows, at] = gated
            squares = squares + gated * gated
        for piece in range(SPAN // 128):
            line = jnp.sum(
                jnp.transpose(squares[piece * 128 : piece * 128 + 128, :]), 0, keepdims=True
            )
            here = slice(block * SPAN + piece * 128, block * SPAN + piece * 128 + 128)
            sum_ref[:, here] = jnp.broadcast_to(line, (sum_ref.shape[0], 128))


def scale_kernel(gated_ref, sum_ref, gain_ref, out_ref, scaled, sem):
    tokens, width = gated_ref.shape
    factor = lax.rsqrt(jnp.sum(sum_ref[...], 0, keepdims=True) / DI + EPSILON)
    copies = []
    for piece in range(tokens // 128):
        rows = slice(piece * 128, piece * 128 + 128)
        column = jnp.transpose(jnp.broadcast_to(factor[:, rows], (128, 128)))
        for tile in range(width // 128):
            at = slice(tile * 128, tile * 128 + 128)
            scaled[rows, at] = (gated_ref[rows, at] * column * gain_ref[:, at]).astype(BF16)
        copy = pltpu.make_async_copy(scaled.at[rows, :], out_ref.at[rows, :], sem.at[piece])
        copy.start()
        copies.append(copy)
    for copy in copies:
        copy.wait()


def whole_block(shape):
    return pl.BlockSpec(shape, lambda *_: (0,) * len(shape))


def params(grid=True, limit=24):
    return pltpu.CompilerParams(
        dimension_semantics=("arbitrary",) if grid else None, vmem_limit_bytes=limit << 20
    )


def cost(flops, moved):
    return pl.CostEstimate(flops=flops, bytes_accessed=moved, transcendentals=0)


SMEM = pl.BlockSpec(memory_space=pltpu.SMEM)
VMEM = pl.BlockSpec(memory_space=pltpu.VMEM)


HBM = pl.BlockSpec(memory_space=pltpu.HBM)


def in_vmem(array):
    return pltpu.with_memory_space_constraint(array, pltpu.VMEM)


def in_hbm(array):
    return pltpu.with_memory_space_constraint(array, pltpu.HBM)


def local(
    x_input, bc_input, z_gate, dt_input, conv_weight_x, conv_weight_bc, conv_bias_x, conv_bias_bc,
    dt_bias, decay_log, skip_scale, norm_gain,
):
    tokens, width = x_input.shape
    heads = dt_input.shape[0]
    blocks = tokens // SPAN
    seq = lax.axis_size("seq")
    tp = lax.axis_size("tp")
    bcw = bc_input.shape[1]
    half = width // 2
    cbx = conv_bias_x.reshape(1, width)
    cbbc = conv_bias_bc.reshape(1, bcw)
    gain = norm_gain.reshape(1, width)

    def block_at(shape, row):
        return pl.BlockSpec(shape, lambda k: (row, 0))

    last = tokens // 8 - 1
    ahead = SPAN // 8 - 1
    weights = [whole_block((4, width)), whole_block((4, bcw)), whole_block((1, width)), whole_block((1, bcw))]
    weight_arrays = (conv_weight_x, conv_weight_bc, cbx, cbbc)
    slab = pltpu.VMEM((width // 128 + 2, SPAN + 8, 128), F32)
    block_xw = pltpu.VMEM((SPAN, width), BF16)
    pair = pltpu.VMEM((2 * heads, tokens), BF16)
    wide = pltpu.VMEM((tokens, width), BF16)
    narrow = pltpu.VMEM((tokens, bcw), BF16)
    state_shape = pltpu.VMEM((STATE, width), F32)
    tail, xc, bcv, w, p, pdev, total, state = pl.pallas_call(
        first_kernel,
        grid=(1,),
        in_specs=[
            block_at((SPAN, width), 1), block_at((8, width), ahead),
            block_at((SPAN, bcw), 1), block_at((8, bcw), ahead),
            block_at((8, width), last), block_at((8, bcw), last),
            whole_block((heads, tokens)), *weights, whole_block((1, heads)), whole_block((1, heads)),
        ],
        out_specs=[VMEM] * 8,
        out_shape=[
            pltpu.VMEM((8, width + bcw), BF16), wide, narrow, pair, pair, pair,
            pltpu.VMEM((8, width), F32), state_shape,
        ],
        scratch_shapes=[slab, block_xw],
        compiler_params=params(limit=16),
        cost_estimate=cost(5_000_000_000, 4 << 20),
        name="first",
    )(
        in_hbm(x_input), in_hbm(x_input), in_hbm(bc_input), in_hbm(bc_input),
        in_hbm(x_input), in_hbm(bc_input), in_hbm(dt_input),
        *(in_hbm(each) for each in weight_arrays),
        in_hbm(dt_bias.reshape(1, heads)), in_hbm(decay_log.reshape(1, heads)),
    )
    halo = lax.ppermute(tail, "seq", [(k, k + 1) for k in range(seq - 1)])

    xc, bcv, state = pl.pallas_call(
        later_kernel,
        in_specs=[VMEM] * 11,
        out_specs=[VMEM] * 3,
        out_shape=[wide, narrow, state_shape],
        scratch_shapes=[slab, block_xw],
        input_output_aliases={8: 2, 9: 0, 10: 1},
        compiler_params=params(False, 16),
        cost_estimate=cost(10_000_000_000, 4 << 20),
        name="later",
    )(x_input, bc_input, *weight_arrays, w, total, state, xc, bcv)

    xc, bcv, message = pl.pallas_call(
        second_kernel,
        in_specs=[VMEM] * 12,
        out_specs=[VMEM] * 3,
        out_shape=[wide, narrow, pltpu.VMEM((2 * STATE, half + 128), BF16)],
        scratch_shapes=[slab, block_xw],
        input_output_aliases={10: 0, 11: 1},
        compiler_params=params(False, 16),
        cost_estimate=cost(5_000_000_000, 4 << 20),
        name="second",
    )(x_input, bc_input, halo, *weight_arrays, w, total, state, xc, bcv)

    sent = lax.all_to_all(message, "seq", 0, 0, tiled=True)

    y = pl.pallas_call(
        middle_kernel,
        in_specs=[VMEM] * 5 + [SMEM],
        out_specs=HBM,
        out_shape=pltpu.HBM((tokens, width), F32),
        scratch_shapes=[
            state_shape, block_xw, pltpu.VMEM((tokens, width), F32),
            pltpu.SemaphoreType.DMA((tokens // SPAN,)),
        ],
        compiler_params=params(False, 24),
        cost_estimate=cost(20_000_000_000, 10 << 20),
        name="middle",
    )(xc, bcv, w, p, total, skip_scale)

    starts = pl.pallas_call(
        prefix_kernel,
        in_specs=[VMEM, HBM],
        out_specs=VMEM,
        out_shape=pltpu.VMEM((2 * STATE, half), BF16),
        compiler_params=params(False, 4),
        cost_estimate=cost(2_000_000_000, 1 << 20),
        name="prefix",
    )(sent, in_hbm(y))
    mine = lax.all_to_all(starts, "seq", 0, 0, tiled=True)

    gated, sums = pl.pallas_call(
        gate_kernel,
        in_specs=[VMEM] * 5,
        out_specs=[VMEM] * 2,
        out_shape=[
            jax.ShapeDtypeStruct((tokens, width), F32), jax.ShapeDtypeStruct((tp, tokens), F32)
        ],
        scratch_shapes=[pltpu.VMEM((STATE, width), BF16)],
        compiler_params=params(False, 16),
        cost_estimate=cost(10_000_000_000, 10 << 20),
        name="gate",
    )(mine, bcv, pdev, in_vmem(y), in_vmem(z_gate))

    all_sums = lax.all_to_all(sums, "tp", 0, 0, tiled=True)

    return pl.pallas_call(
        scale_kernel,
        in_specs=[VMEM] * 3,
        out_specs=HBM,
        out_shape=pltpu.HBM((tokens, width), BF16),
        scratch_shapes=[
            pltpu.VMEM((tokens, width), BF16), pltpu.SemaphoreType.DMA((tokens // 128,))
        ],
        compiler_params=params(False, 16),
        cost_estimate=cost(5_000_000_000, 6 << 20),
        name="scale",
    )(gated, all_sums, gain)


def solution(mesh):
    return jax.shard_map(
        local,
        mesh=mesh,
        in_specs=(
            P("seq", "tp"), P("seq", "tp"), P("seq", "tp"), P("tp", "seq"),
            P(None, "tp"), P(None, "tp"),
            P("tp"), P("tp"), P("tp"), P("tp"), P("tp"), P("tp"),
        ),
        out_specs=P("seq", "tp"),
        check_vma=False,
    )
```

```python
import functools

import jax
import jax.numpy as jnp
from jax import lax
from jax.experimental import pallas as pl
from jax.experimental.pallas import tpu as pltpu
from jax.sharding import PartitionSpec as P

HEAD_DIM = 64
STATE = 128
SPAN = 256
DI = 8192
EPSILON = 1e-05

F32 = jnp.float32
BF16 = jnp.bfloat16


def column_of(line):
    count = line.shape[1]
    row = lax.broadcasted_iota(jnp.int32, (count, count), 0)
    lane = lax.broadcasted_iota(jnp.int32, (count, count), 1)
    return jnp.sum(jnp.where(row == lane, line, 0.0), 1, keepdims=True)


def head_mask(heads, width):
    row = lax.broadcasted_iota(jnp.int32, (heads, width), 0)
    lane = lax.broadcasted_iota(jnp.int32, (heads, width), 1)
    return lane // HEAD_DIM == row


def expander(heads, width):
    one_hot = jnp.where(head_mask(heads, width), 1.0, 0.0)
    return jnp.concatenate([one_hot, one_hot], 0).astype(BF16)


def high_low(value):
    high = value.astype(BF16).astype(F32)
    return jnp.concatenate([high, value - high], 0).astype(BF16)


def spread(pair, one_hot):
    return lax.dot_general(pair, one_hot, (((0,), (0,)), ((), ())), preferred_element_type=F32)


def half_silu(half):
    return half + half * jnp.tanh(half)


def conv_tile(slab, tile, x_tile, halo_tile, weight, bias):
    rows = x_tile.shape[0]
    slab[tile, 0:8, :] = halo_tile.astype(F32)
    slab[tile, 8 : 8 + rows, :] = x_tile.astype(F32)
    total = bias
    for tap in range(4):
        total = total + slab[tile, 5 + tap : 5 + tap + rows, :] * weight[tap : tap + 1, :]
    return half_silu(total).astype(BF16)


def conv_group(slab, halo_bc, bc, cwbc, cbbc, lanes, out, rows):
    out[rows, :] = conv_tile(
        slab, 0, bc[:, lanes], halo_bc[:, lanes], cwbc[:, lanes].astype(F32) * 0.5, cbbc[:, lanes] * 0.5
    )


def block_state(slab, xw, halo_x, halo_bc, x, bc, cwx, cwbc, cbx, cbbc, pair, xc_out, b_out, rows):
    width = x.shape[1]
    heads = width // HEAD_DIM
    tiles = width // 128
    conv_group(slab.at[tiles : tiles + 1], halo_bc, bc, cwbc, cbbc, slice(0, STATE), b_out, rows)
    weight = spread(pair, expander(heads, width))
    for tile in range(tiles):
        at = slice(tile * 128, tile * 128 + 128)
        conv = conv_tile(
            slab, tile, x[:, at], halo_x[:, at], cwx[:, at].astype(F32) * 0.5, cbx[:, at] * 0.5
        )
        xc_out[rows, at] = conv
        xw[:, at] = (conv.astype(F32) * weight[:, at]).astype(BF16)
    return lax.dot_general(
        b_out[rows, :], xw[...], (((0,), (0,)), ((), ())), preferred_element_type=F32
    )


def first_kernel(
    x_hbm, bc_hbm, dt_hbm, bias_hbm, decay_hbm, cwx_hbm, cwbc_hbm, cbx_hbm, cbbc_hbm,
    x, bc, tail_ref, xc_ref, b_ref, w_ref, cum_ref, total_ref, state_ref,
    slab, xw, dt, bias, decay, cwx, cwbc, cbx, cbbc, sem,
):
    tokens, width = x.shape
    heads = dt.shape[0]
    second = slice(SPAN - 8, 2 * SPAN)
    final = slice(tokens - 8, tokens)
    copies = []
    for source, target in (
        (dt_hbm, dt),
        (bias_hbm, bias),
        (decay_hbm, decay),
        (x_hbm.at[second, :], x.at[second, :]),
        (bc_hbm.at[second, :], bc.at[second, :]),
        (cwx_hbm, cwx),
        (cwbc_hbm, cwbc),
        (cbx_hbm, cbx),
        (cbbc_hbm, cbbc),
        (x_hbm.at[final, :], tail_ref.at[:, 0:width]),
        (bc_hbm.at[final, :], tail_ref.at[:, width:]),
        (x_hbm.at[2 * SPAN :, :], x.at[2 * SPAN :, :]),
        (bc_hbm.at[2 * SPAN :, :], bc.at[2 * SPAN :, :]),
        (x_hbm.at[: SPAN - 8, :], x.at[: SPAN - 8, :]),
        (bc_hbm.at[: SPAN - 8, :], bc.at[: SPAN - 8, :]),
    ):
        copy = pltpu.make_async_copy(source, target, sem.at[len(copies)])
        copy.start()
        copies.append(copy)
    for copy in copies[0:3]:
        copy.wait()
    rate = jnp.exp(column_of(decay[...]))
    raw = dt[...].astype(F32) + column_of(bias[...])
    size = jnp.maximum(raw, 0.0) + jnp.log(1.0 + jnp.exp(-jnp.abs(raw)))
    cum = -rate * size
    position = lax.broadcasted_iota(jnp.int32, (heads, tokens), 1) & (SPAN - 1)
    shift = 1
    while shift < SPAN:
        cum = cum + jnp.where(position >= shift, pltpu.roll(cum, shift, 1), 0.0)
        shift *= 2
    cum_ref[...] = cum
    w_ref[...] = high_low(jnp.exp(-cum) * size)
    mask = head_mask(heads, width)
    sub = lax.broadcasted_iota(jnp.int32, (8, width), 0)
    table = jnp.zeros((8, width), F32)
    for block in range(tokens // SPAN):
        last = cum[:, block * SPAN + SPAN - 1 : block * SPAN + SPAN]
        row = jnp.sum(jnp.where(mask, jnp.exp(last), 0.0), 0, keepdims=True)
        table = jnp.where(sub == block, row, table)
    total_ref[...] = table
    for copy in copies[3:9]:
        copy.wait()
    at = slice(SPAN, 2 * SPAN)
    ahead = slice(SPAN - 8, SPAN)
    added = block_state(
        slab, xw, x.at[ahead, :], bc.at[ahead, :], x.at[at, :], bc.at[at, :],
        cwx, cwbc, cbx, cbbc, w_ref[:, at], xc_ref, b_ref, at,
    )
    state_ref[...] = added * total_ref[1:2, :]
    for copy in copies[9:]:
        copy.wait()


def later_kernel(
    x_ref, bc_ref, cwx_ref, cwbc_ref, cbx_ref, cbbc_ref, w_ref, total_ref, state_in, xc_in, b_in,
    xc_ref, b_ref, state_ref,
    slab, xw,
):
    tokens = x_ref.shape[0]
    for block in range(2, tokens // SPAN):
        at = slice(block * SPAN, block * SPAN + SPAN)
        ahead = slice(block * SPAN - 8, block * SPAN)
        added = block_state(
            slab, xw, x_ref.at[ahead, :], bc_ref.at[ahead, :], x_ref.at[at, :], bc_ref.at[at, :],
            cwx_ref, cwbc_ref, cbx_ref, cbbc_ref, w_ref[:, at], xc_ref, b_ref, at,
        )
        previous = state_in if block == 2 else state_ref
        state_ref[...] = (previous[...] + added) * total_ref[block : block + 1, :]


def second_kernel(
    x_ref, bc_ref, halo_ref, cwx_ref, cwbc_ref, cbx_ref, cbbc_ref, w_ref, total_ref, state_ref,
    xc_in, b_in,
    xc_ref, b_ref, message_ref,
    slab, xw,
):
    width = x_ref.shape[1]
    half = width // 2
    at = slice(0, SPAN)
    added = block_state(
        slab, xw, halo_ref.at[:, 0:width], halo_ref.at[:, width : width + 2 * STATE],
        x_ref.at[at, :], bc_ref.at[at, :], cwx_ref, cwbc_ref, cbx_ref, cbbc_ref,
        w_ref[:, at], xc_ref, b_ref, at,
    )
    table = total_ref[...]
    decay = table[0:1, :] * (table[1:2, :] * table[2:3, :] * table[3:4, :])
    everything = state_ref[...] + added * decay
    high = decay.astype(BF16).astype(F32)
    low = decay - high
    sub = lax.broadcasted_iota(jnp.int32, (16, 128), 0)
    extra = jnp.zeros((16, 128), F32)
    for side in range(2):
        for tile in range(4):
            at = slice(side * half + tile * 128, side * half + tile * 128 + 128)
            extra = jnp.where(sub == side * 8 + tile, high[:, at], extra)
            extra = jnp.where(sub == side * 8 + 4 + tile, low[:, at], extra)
    extra = extra.astype(BF16)
    for group in range(STATE // 8):
        rows = everything[group * 8 : group * 8 + 8, :]
        both = jnp.concatenate([rows[:, 0:half], rows[:, half:width]], 0)
        message_ref[group * 16 : group * 16 + 16, 0:half] = both.astype(BF16)
        message_ref[group * 16 : group * 16 + 16, half : half + 128] = extra


def prefix_kernel(message_ref, after_ref, out_ref):
    rows, width = out_ref.shape

    def decay_of(extra):
        return jnp.concatenate(
            [
                jnp.broadcast_to(extra[q : q + 1, :] + extra[q + 4 : q + 5, :], (8, 128))
                for q in range(width // 128)
            ],
            1,
        )

    carried = jnp.zeros((8, width), F32)
    for pair in range(rows // 16):
        at = slice(pair * 16, pair * 16 + 16)
        both = message_ref[at, :].astype(F32)
        middle = decay_of(both[0:8, width:]) * carried + both[0:8, 0:width]
        out_ref[at, :] = jnp.concatenate([carried, middle], 0).astype(BF16)
        carried = decay_of(both[8:16, width:]) * middle + both[8:16, 0:width]


def middle_kernel(
    xc_ref, b_ref, bc_ref, halo_ref, cwbc_ref, cbbc_ref, w_ref, cum_ref, total_ref, skip_ref,
    y_ref, c_out,
    state, xw, y, slab, c_ref, sem,
):
    tokens, width = xc_ref.shape
    heads = width // HEAD_DIM
    head_row = lax.broadcasted_iota(jnp.int32, (1, width), 1) // HEAD_DIM
    skip = jnp.zeros((1, width), F32)
    for head in range(heads):
        skip = jnp.where(head_row == head, skip_ref[head], skip)
    one_hot = expander(heads, width)
    row = lax.broadcasted_iota(jnp.int32, (SPAN, SPAN), 0)
    lane = lax.broadcasted_iota(jnp.int32, (SPAN, SPAN), 1)
    copies = []
    for block in range(tokens // SPAN):
        at = slice(block * SPAN, block * SPAN + SPAN)
        if block == 0:
            halo_bc = halo_ref.at[:, width : width + 2 * STATE]
        else:
            halo_bc = bc_ref.at[block * SPAN - 8 : block * SPAN, :]
        conv_group(
            slab, halo_bc, bc_ref.at[at, :], cwbc_ref, cbbc_ref, slice(STATE, 2 * STATE), c_ref, at
        )
        b_part = b_ref[at, :]
        c_part = c_ref[at, :]
        scores = lax.dot_general(
            c_part, b_part, (((1,), (1,)), ((), ())), preferred_element_type=F32
        )
        masked = jnp.where(row >= lane, scores, 0.0).astype(BF16)
        xw[...] = (xc_ref[at, :].astype(F32) * spread(w_ref[:, at], one_hot)).astype(BF16)
        total = jnp.dot(masked, xw[...], preferred_element_type=F32)
        if block > 0:
            total = total + jnp.dot(
                c_part, state[...].astype(BF16), preferred_element_type=F32
            )
        grown = spread(high_low(jnp.exp(cum_ref[:, at])), one_hot)
        y[at, :] = grown * total + skip * xc_ref[at, :].astype(F32)
        copy = pltpu.make_async_copy(y.at[at, :], y_ref.at[at, :], sem.at[block])
        copy.start()
        copies.append(copy)
        if (block + 1) * SPAN < tokens:
            added = lax.dot_general(
                b_part, xw[...], (((0,), (0,)), ((), ())), preferred_element_type=F32
            )
            if block > 0:
                added = added + state[...]
            state[...] = added * total_ref[block : block + 1, :]
    copy = pltpu.make_async_copy(c_ref, c_out, sem.at[len(copies)])
    copy.start()
    copies.append(copy)
    for copy in copies:
        copy.wait()


def gate_kernel(start_ref, c_ref, cum_ref, y_ref, z_ref, gated_ref, sum_ref, start):
    tokens, width = y_ref.shape
    heads = width // HEAD_DIM
    half = width // 2
    for pair in range(STATE // 16):
        block = start_ref[pair * 32 : pair * 32 + 32, :].astype(F32)
        for side in range(2):
            rows = jnp.concatenate(
                [block[side * 8 : side * 8 + 8, :], block[16 + side * 8 : 24 + side * 8, :]], 0
            )
            start[pair * 16 : pair * 16 + 16, side * half : side * half + half] = rows.astype(BF16)
    one_hot = expander(heads, width)
    before = jnp.zeros((heads, 1), F32)
    for block in range(tokens // SPAN):
        rows = slice(block * SPAN, block * SPAN + SPAN)
        cum = cum_ref[:, rows]
        product = jnp.dot(c_ref[rows, :], start[...], preferred_element_type=F32)
        grown = spread(high_low(jnp.exp(cum + before)), one_hot)
        before = before + cum[:, SPAN - 1 : SPAN]
        squares = jnp.zeros((SPAN, 128), F32)
        for tile in range(width // 128):
            at = slice(tile * 128, tile * 128 + 128)
            gated = (y_ref[rows, at] + grown[:, at] * product[:, at]) * half_silu(
                z_ref[rows, at].astype(F32) * 0.5
            )
            gated_ref[rows, at] = gated
            squares = squares + gated * gated
        for piece in range(SPAN // 128):
            line = jnp.sum(
                jnp.transpose(squares[piece * 128 : piece * 128 + 128, :]), 0, keepdims=True
            )
            here = slice(block * SPAN + piece * 128, block * SPAN + piece * 128 + 128)
            sum_ref[:, here] = jnp.broadcast_to(line, (sum_ref.shape[0], 128))


def scale_kernel(gated_ref, sum_ref, gain_ref, out_ref, scaled, sem):
    tokens, width = gated_ref.shape
    factor = lax.rsqrt(jnp.sum(sum_ref[...], 0, keepdims=True) / DI + EPSILON)
    copies = []
    for piece in range(tokens // 128):
        rows = slice(piece * 128, piece * 128 + 128)
        column = jnp.transpose(jnp.broadcast_to(factor[:, rows], (128, 128)))
        for tile in range(width // 128):
            at = slice(tile * 128, tile * 128 + 128)
            scaled[rows, at] = (gated_ref[rows, at] * column * gain_ref[:, at]).astype(BF16)
        copy = pltpu.make_async_copy(scaled.at[rows, :], out_ref.at[rows, :], sem.at[piece])
        copy.start()
        copies.append(copy)
    for copy in copies:
        copy.wait()


def whole_block(shape):
    return pl.BlockSpec(shape, lambda *_: (0,) * len(shape))


def params(grid=True, limit=24):
    return pltpu.CompilerParams(
        dimension_semantics=("arbitrary",) if grid else None, vmem_limit_bytes=limit << 20
    )


def cost(flops, moved):
    return pl.CostEstimate(flops=flops, bytes_accessed=moved, transcendentals=0)


SMEM = pl.BlockSpec(memory_space=pltpu.SMEM)
VMEM = pl.BlockSpec(memory_space=pltpu.VMEM)


HBM = pl.BlockSpec(memory_space=pltpu.HBM)


def in_vmem(array):
    return pltpu.with_memory_space_constraint(array, pltpu.VMEM)


def in_hbm(array):
    return pltpu.with_memory_space_constraint(array, pltpu.HBM)


def local(
    x_input, bc_input, z_gate, dt_input, conv_weight_x, conv_weight_bc, conv_bias_x, conv_bias_bc,
    dt_bias, decay_log, skip_scale, norm_gain,
):
    tokens, width = x_input.shape
    heads = dt_input.shape[0]
    blocks = tokens // SPAN
    seq = lax.axis_size("seq")
    tp = lax.axis_size("tp")
    bcw = bc_input.shape[1]
    half = width // 2
    cbx = conv_bias_x.reshape(1, width)
    cbbc = conv_bias_bc.reshape(1, bcw)
    gain = norm_gain.reshape(1, width)

    weight_arrays = (conv_weight_x, conv_weight_bc, cbx, cbbc)
    slab = pltpu.VMEM((width // 128 + 1, SPAN + 8, 128), F32)
    block_xw = pltpu.VMEM((SPAN, width), BF16)
    wide = pltpu.VMEM((tokens, width), BF16)
    narrow = pltpu.VMEM((tokens, STATE), BF16)
    state_shape = pltpu.VMEM((STATE, width), F32)
    x_near, bc_near, tail, xc, b_conv, w, cum, total, state = pl.pallas_call(
        first_kernel,
        in_specs=[HBM] * 9,
        out_specs=[VMEM] * 9,
        out_shape=[
            wide, pltpu.VMEM((tokens, bcw), BF16),
            pltpu.VMEM((8, width + bcw), BF16), wide, narrow,
            pltpu.VMEM((2 * heads, tokens), BF16), pltpu.VMEM((heads, tokens), F32),
            pltpu.VMEM((8, width), F32), state_shape,
        ],
        scratch_shapes=[
            slab, block_xw, pltpu.VMEM((heads, tokens), BF16), pltpu.VMEM((1, heads), F32), pltpu.VMEM((1, heads), F32),
            pltpu.VMEM((4, width), BF16), pltpu.VMEM((4, bcw), BF16),
            pltpu.VMEM((1, width), F32), pltpu.VMEM((1, bcw), F32),
            pltpu.SemaphoreType.DMA((15,)),
        ],
        compiler_params=params(False, 16),
        cost_estimate=cost(5_000_000_000, 4 << 20),
        name="first",
    )(
        *(
            in_hbm(each)
            for each in (
                x_input, bc_input, dt_input, dt_bias.reshape(1, heads),
                decay_log.reshape(1, heads), *weight_arrays,
            )
        )
    )
    halo = lax.ppermute(tail, "seq", [(k, k + 1) for k in range(seq - 1)])

    xc, b_conv, state = pl.pallas_call(
        later_kernel,
        in_specs=[VMEM] * 11,
        out_specs=[VMEM] * 3,
        out_shape=[wide, narrow, state_shape],
        scratch_shapes=[slab, block_xw],
        input_output_aliases={8: 2, 9: 0, 10: 1},
        compiler_params=params(False, 16),
        cost_estimate=cost(10_000_000_000, 4 << 20),
        name="later",
    )(x_near, bc_near, *weight_arrays, w, total, state, xc, b_conv)

    xc, b_conv, message = pl.pallas_call(
        second_kernel,
        in_specs=[VMEM] * 12,
        out_specs=[VMEM] * 3,
        out_shape=[wide, narrow, pltpu.VMEM((2 * STATE, half + 128), BF16)],
        scratch_shapes=[slab, block_xw],
        input_output_aliases={10: 0, 11: 1},
        compiler_params=params(False, 16),
        cost_estimate=cost(5_000_000_000, 4 << 20),
        name="second",
    )(x_near, bc_near, halo, *weight_arrays, w, total, state, xc, b_conv)

    sent = lax.all_to_all(message, "seq", 0, 0, tiled=True)

    y, c_conv = pl.pallas_call(
        middle_kernel,
        in_specs=[VMEM] * 9 + [SMEM],
        out_specs=[HBM, HBM],
        out_shape=[pltpu.HBM((tokens, width), F32), pltpu.HBM((tokens, STATE), BF16)],
        scratch_shapes=[
            state_shape, block_xw, pltpu.VMEM((tokens, width), F32),
            pltpu.VMEM((1, SPAN + 8, 128), F32), narrow,
            pltpu.SemaphoreType.DMA((tokens // SPAN + 1,)),
        ],
        compiler_params=params(False, 24),
        cost_estimate=cost(20_000_000_000, 10 << 20),
        name="middle",
    )(xc, b_conv, bc_input, halo, conv_weight_bc, cbbc, w, cum, total, skip_scale)

    starts = pl.pallas_call(
        prefix_kernel,
        in_specs=[VMEM, HBM],
        out_specs=VMEM,
        out_shape=pltpu.VMEM((2 * STATE, half), BF16),
        compiler_params=params(False, 4),
        cost_estimate=cost(2_000_000_000, 1 << 20),
        name="prefix",
    )(sent, in_hbm(y))
    mine = lax.all_to_all(starts, "seq", 0, 0, tiled=True)

    gated, sums = pl.pallas_call(
        gate_kernel,
        in_specs=[VMEM] * 5,
        out_specs=[VMEM] * 2,
        out_shape=[
            jax.ShapeDtypeStruct((tokens, width), F32), jax.ShapeDtypeStruct((tp, tokens), F32)
        ],
        scratch_shapes=[pltpu.VMEM((STATE, width), BF16)],
        compiler_params=params(False, 16),
        cost_estimate=cost(10_000_000_000, 10 << 20),
        name="gate",
    )(mine, in_vmem(c_conv), cum, in_vmem(y), in_vmem(z_gate))

    all_sums = lax.all_to_all(sums, "tp", 0, 0, tiled=True)

    return pl.pallas_call(
        scale_kernel,
        in_specs=[VMEM] * 3,
        out_specs=HBM,
        out_shape=pltpu.HBM((tokens, width), BF16),
        scratch_shapes=[
            pltpu.VMEM((tokens, width), BF16), pltpu.SemaphoreType.DMA((tokens // 128,))
        ],
        compiler_params=params(False, 16),
        cost_estimate=cost(5_000_000_000, 6 << 20),
        name="scale",
    )(gated, all_sums, gain)


def solution(mesh):
    return jax.shard_map(
        local,
        mesh=mesh,
        in_specs=(
            P("seq", "tp"), P("seq", "tp"), P("seq", "tp"), P("tp", "seq"),
            P(None, "tp"), P(None, "tp"),
            P("tp"), P("tp"), P("tp"), P("tp"), P("tp"), P("tp"),
        ),
        out_specs=P("seq", "tp"),
        check_vma=False,
    )
```

```python
import functools

import jax
import jax.numpy as jnp
from jax import lax
from jax.experimental import pallas as pl
from jax.experimental.pallas import tpu as pltpu
from jax.sharding import PartitionSpec as P

HEAD_DIM = 64
STATE = 128
SPAN = 256
DI = 8192
EPSILON = 1e-05

F32 = jnp.float32
BF16 = jnp.bfloat16


def column_of(line):
    count = line.shape[1]
    row = lax.broadcasted_iota(jnp.int32, (count, count), 0)
    lane = lax.broadcasted_iota(jnp.int32, (count, count), 1)
    return jnp.sum(jnp.where(row == lane, line, 0.0), 1, keepdims=True)


def head_mask(heads, width):
    row = lax.broadcasted_iota(jnp.int32, (heads, width), 0)
    lane = lax.broadcasted_iota(jnp.int32, (heads, width), 1)
    return lane // HEAD_DIM == row


def expander(heads, width):
    one_hot = jnp.where(head_mask(heads, width), 1.0, 0.0)
    return jnp.concatenate([one_hot, one_hot], 0).astype(BF16)


def high_low(value):
    high = value.astype(BF16).astype(F32)
    return jnp.concatenate([high, value - high], 0).astype(BF16)


def spread(pair, one_hot):
    return lax.dot_general(pair, one_hot, (((0,), (0,)), ((), ())), preferred_element_type=F32)


def half_silu(half):
    return half + half * jnp.tanh(half)


def conv_tile(slab, tile, x_tile, halo_tile, weight, bias):
    rows = x_tile.shape[0]
    slab[tile, 0:8, :] = halo_tile.astype(F32)
    slab[tile, 8 : 8 + rows, :] = x_tile.astype(F32)
    total = bias
    for tap in range(4):
        total = total + slab[tile, 5 + tap : 5 + tap + rows, :] * weight[tap : tap + 1, :]
    return half_silu(total).astype(BF16)


def conv_group(slab, halo_bc, bc, cwbc, cbbc, lanes, out, rows):
    out[rows, :] = conv_tile(
        slab, 0, bc[:, lanes], halo_bc[:, lanes], cwbc[:, lanes].astype(F32) * 0.5, cbbc[:, lanes] * 0.5
    )


def block_state(slab, xw, halo_x, halo_bc, x, bc, cwx, cwbc, cbx, cbbc, pair, xc_out, b_out, rows):
    width = x.shape[1]
    heads = width // HEAD_DIM
    tiles = width // 128
    conv_group(slab.at[tiles : tiles + 1], halo_bc, bc, cwbc, cbbc, slice(0, STATE), b_out, rows)
    weight = spread(pair, expander(heads, width))
    for tile in range(tiles):
        at = slice(tile * 128, tile * 128 + 128)
        conv = conv_tile(
            slab, tile, x[:, at], halo_x[:, at], cwx[:, at].astype(F32) * 0.5, cbx[:, at] * 0.5
        )
        xc_out[rows, at] = conv
        xw[:, at] = (conv.astype(F32) * weight[:, at]).astype(BF16)
    return lax.dot_general(
        b_out[rows, :], xw[...], (((0,), (0,)), ((), ())), preferred_element_type=F32
    )


def first_kernel(
    x_hbm, bc_hbm, dt_hbm, bias_hbm, decay_hbm, cwx_hbm, cwbc_hbm, cbx_hbm, cbbc_hbm,
    x, bc, tail_ref, xc_ref, b_ref, w_ref, cum_ref, total_ref, state_ref,
    slab, xw, dt, bias, decay, cwx, cwbc, cbx, cbbc, sem,
):
    tokens, width = x.shape
    heads = dt.shape[0]
    second = slice(SPAN - 8, 2 * SPAN)
    final = slice(tokens - 8, tokens)
    copies = []
    for source, target in (
        (dt_hbm, dt),
        (bias_hbm, bias),
        (decay_hbm, decay),
        (x_hbm.at[second, :], x.at[second, :]),
        (bc_hbm.at[second, :], bc.at[second, :]),
        (cwx_hbm, cwx),
        (cwbc_hbm, cwbc),
        (cbx_hbm, cbx),
        (cbbc_hbm, cbbc),
        (x_hbm.at[final, :], tail_ref.at[:, 0:width]),
        (bc_hbm.at[final, :], tail_ref.at[:, width:]),
        (x_hbm.at[2 * SPAN :, :], x.at[2 * SPAN :, :]),
        (bc_hbm.at[2 * SPAN :, :], bc.at[2 * SPAN :, :]),
        (x_hbm.at[: SPAN - 8, :], x.at[: SPAN - 8, :]),
        (bc_hbm.at[: SPAN - 8, :], bc.at[: SPAN - 8, :]),
    ):
        copy = pltpu.make_async_copy(source, target, sem.at[len(copies)])
        copy.start()
        copies.append(copy)
    for copy in copies[0:3]:
        copy.wait()
    rate = jnp.exp(column_of(decay[...]))
    raw = dt[...].astype(F32) + column_of(bias[...])
    size = jnp.maximum(raw, 0.0) + jnp.log(1.0 + jnp.exp(-jnp.abs(raw)))
    cum = -rate * size
    position = lax.broadcasted_iota(jnp.int32, (heads, tokens), 1) & (SPAN - 1)
    shift = 1
    while shift < SPAN:
        cum = cum + jnp.where(position >= shift, pltpu.roll(cum, shift, 1), 0.0)
        shift *= 2
    cum_ref[...] = cum
    w_ref[...] = high_low(jnp.exp(-cum) * size)
    mask = head_mask(heads, width)
    sub = lax.broadcasted_iota(jnp.int32, (8, width), 0)
    table = jnp.zeros((8, width), F32)
    for block in range(tokens // SPAN):
        last = cum[:, block * SPAN + SPAN - 1 : block * SPAN + SPAN]
        row = jnp.sum(jnp.where(mask, jnp.exp(last), 0.0), 0, keepdims=True)
        table = jnp.where(sub == block, row, table)
    total_ref[...] = table
    for copy in copies[3:9]:
        copy.wait()
    at = slice(SPAN, 2 * SPAN)
    ahead = slice(SPAN - 8, SPAN)
    added = block_state(
        slab, xw, x.at[ahead, :], bc.at[ahead, :], x.at[at, :], bc.at[at, :],
        cwx, cwbc, cbx, cbbc, w_ref[:, at], xc_ref, b_ref, at,
    )
    state_ref[...] = added * total_ref[1:2, :]
    for copy in copies[9:]:
        copy.wait()


def later_kernel(
    x_ref, bc_ref, cwx_ref, cwbc_ref, cbx_ref, cbbc_ref, w_ref, total_ref, state_in, xc_in, b_in,
    xc_ref, b_ref, state_ref,
    slab, xw,
):
    tokens = x_ref.shape[0]
    for block in range(2, tokens // SPAN):
        at = slice(block * SPAN, block * SPAN + SPAN)
        ahead = slice(block * SPAN - 8, block * SPAN)
        added = block_state(
            slab.at[block % 2], xw.at[block % 2],
            x_ref.at[ahead, :], bc_ref.at[ahead, :], x_ref.at[at, :], bc_ref.at[at, :],
            cwx_ref, cwbc_ref, cbx_ref, cbbc_ref, w_ref[:, at], xc_ref, b_ref, at,
        )
        previous = state_in if block == 2 else state_ref
        state_ref[...] = (previous[...] + added) * total_ref[block : block + 1, :]


def second_kernel(
    x_ref, bc_ref, halo_ref, cwx_ref, cwbc_ref, cbx_ref, cbbc_ref, w_ref, total_ref, state_ref,
    xc_in, b_in,
    xc_ref, b_ref, message_ref,
    slab, xw,
):
    width = x_ref.shape[1]
    half = width // 2
    at = slice(0, SPAN)
    added = block_state(
        slab, xw, halo_ref.at[:, 0:width], halo_ref.at[:, width : width + 2 * STATE],
        x_ref.at[at, :], bc_ref.at[at, :], cwx_ref, cwbc_ref, cbx_ref, cbbc_ref,
        w_ref[:, at], xc_ref, b_ref, at,
    )
    table = total_ref[...]
    decay = table[0:1, :] * (table[1:2, :] * table[2:3, :] * table[3:4, :])
    everything = state_ref[...] + added * decay
    high = decay.astype(BF16).astype(F32)
    low = decay - high
    sub = lax.broadcasted_iota(jnp.int32, (16, 128), 0)
    extra = jnp.zeros((16, 128), F32)
    for side in range(2):
        for tile in range(4):
            at = slice(side * half + tile * 128, side * half + tile * 128 + 128)
            extra = jnp.where(sub == side * 8 + tile, high[:, at], extra)
            extra = jnp.where(sub == side * 8 + 4 + tile, low[:, at], extra)
    extra = extra.astype(BF16)
    for group in range(STATE // 8):
        rows = everything[group * 8 : group * 8 + 8, :]
        both = jnp.concatenate([rows[:, 0:half], rows[:, half:width]], 0)
        message_ref[group * 16 : group * 16 + 16, 0:half] = both.astype(BF16)
        message_ref[group * 16 : group * 16 + 16, half : half + 128] = extra


def prefix_kernel(message_ref, after_ref, out_ref):
    rows, width = out_ref.shape

    def decay_of(extra):
        return jnp.concatenate(
            [
                jnp.broadcast_to(extra[q : q + 1, :] + extra[q + 4 : q + 5, :], (8, 128))
                for q in range(width // 128)
            ],
            1,
        )

    carried = jnp.zeros((8, width), F32)
    for pair in range(rows // 16):
        at = slice(pair * 16, pair * 16 + 16)
        both = message_ref[at, :].astype(F32)
        middle = decay_of(both[0:8, width:]) * carried + both[0:8, 0:width]
        out_ref[at, :] = jnp.concatenate([carried, middle], 0).astype(BF16)
        carried = decay_of(both[8:16, width:]) * middle + both[8:16, 0:width]


def middle_kernel(
    xc_ref, b_ref, bc_ref, halo_ref, cwbc_ref, cbbc_ref, w_ref, cum_ref, total_ref, skip_ref,
    y_ref, c_out,
    state, xw, y, slab, c_ref, sem,
):
    tokens, width = xc_ref.shape
    heads = width // HEAD_DIM
    head_row = lax.broadcasted_iota(jnp.int32, (1, width), 1) // HEAD_DIM
    skip = jnp.zeros((1, width), F32)
    for head in range(heads):
        skip = jnp.where(head_row == head, skip_ref[head], skip)
    one_hot = expander(heads, width)
    row = lax.broadcasted_iota(jnp.int32, (SPAN, SPAN), 0)
    lane = lax.broadcasted_iota(jnp.int32, (SPAN, SPAN), 1)
    copies = []
    for block in range(tokens // SPAN):
        at = slice(block * SPAN, block * SPAN + SPAN)
        if block == 0:
            halo_bc = halo_ref.at[:, width : width + 2 * STATE]
        else:
            halo_bc = bc_ref.at[block * SPAN - 8 : block * SPAN, :]
        conv_group(
            slab, halo_bc, bc_ref.at[at, :], cwbc_ref, cbbc_ref, slice(STATE, 2 * STATE), c_ref, at
        )
        b_part = b_ref[at, :]
        c_part = c_ref[at, :]
        scores = lax.dot_general(
            c_part, b_part, (((1,), (1,)), ((), ())), preferred_element_type=F32
        )
        masked = jnp.where(row >= lane, scores, 0.0).astype(BF16)
        xw[...] = (xc_ref[at, :].astype(F32) * spread(w_ref[:, at], one_hot)).astype(BF16)
        total = jnp.dot(masked, xw[...], preferred_element_type=F32)
        if block > 0:
            total = total + jnp.dot(
                c_part, state[...].astype(BF16), preferred_element_type=F32
            )
        grown = spread(high_low(jnp.exp(cum_ref[:, at])), one_hot)
        y[at, :] = grown * total + skip * xc_ref[at, :].astype(F32)
        copy = pltpu.make_async_copy(y.at[at, :], y_ref.at[at, :], sem.at[block])
        copy.start()
        copies.append(copy)
        if (block + 1) * SPAN < tokens:
            added = lax.dot_general(
                b_part, xw[...], (((0,), (0,)), ((), ())), preferred_element_type=F32
            )
            if block > 0:
                added = added + state[...]
            state[...] = added * total_ref[block : block + 1, :]
    copy = pltpu.make_async_copy(c_ref, c_out, sem.at[len(copies)])
    copy.start()
    copies.append(copy)
    for copy in copies:
        copy.wait()


def gate_kernel(start_ref, c_ref, cum_ref, y_ref, z_ref, gated_ref, sum_ref, start):
    tokens, width = y_ref.shape
    heads = width // HEAD_DIM
    half = width // 2
    for pair in range(STATE // 16):
        block = start_ref[pair * 32 : pair * 32 + 32, :].astype(F32)
        for side in range(2):
            rows = jnp.concatenate(
                [block[side * 8 : side * 8 + 8, :], block[16 + side * 8 : 24 + side * 8, :]], 0
            )
            start[pair * 16 : pair * 16 + 16, side * half : side * half + half] = rows.astype(BF16)
    one_hot = expander(heads, width)
    before = jnp.zeros((heads, 1), F32)
    for block in range(tokens // SPAN):
        rows = slice(block * SPAN, block * SPAN + SPAN)
        cum = cum_ref[:, rows]
        pair = high_low(jnp.exp(cum + before))
        before = before + cum[:, SPAN - 1 : SPAN]
        squares = jnp.zeros((SPAN, 128), F32)
        for group in range(width // 256):
            lanes = slice(group * 256, group * 256 + 256)
            product = jnp.dot(c_ref[rows, :], start[:, lanes], preferred_element_type=F32)
            arrived = product * spread(pair, one_hot[:, lanes])
            for tile in range(2):
                at = slice(lanes.start + tile * 128, lanes.start + tile * 128 + 128)
                here = slice(tile * 128, tile * 128 + 128)
                gated = (y_ref[rows, at] + arrived[:, here]) * half_silu(
                    z_ref[rows, at].astype(F32) * 0.5
                )
                gated_ref[rows, at] = gated
                squares = squares + gated * gated
        for piece in range(SPAN // 128):
            line = jnp.sum(
                jnp.transpose(squares[piece * 128 : piece * 128 + 128, :]), 0, keepdims=True
            )
            here = slice(block * SPAN + piece * 128, block * SPAN + piece * 128 + 128)
            sum_ref[:, here] = jnp.broadcast_to(line, (sum_ref.shape[0], 128))


def scale_kernel(gated_ref, sum_ref, gain_ref, out_ref, scaled, sem):
    tokens, width = gated_ref.shape
    factor = lax.rsqrt(jnp.sum(sum_ref[...], 0, keepdims=True) / DI + EPSILON)
    copies = []
    for piece in range(tokens // 128):
        rows = slice(piece * 128, piece * 128 + 128)
        column = jnp.transpose(jnp.broadcast_to(factor[:, rows], (128, 128)))
        for tile in range(width // 128):
            at = slice(tile * 128, tile * 128 + 128)
            scaled[rows, at] = (gated_ref[rows, at] * column * gain_ref[:, at]).astype(BF16)
        copy = pltpu.make_async_copy(scaled.at[rows, :], out_ref.at[rows, :], sem.at[piece])
        copy.start()
        copies.append(copy)
    for copy in copies:
        copy.wait()


def whole_block(shape):
    return pl.BlockSpec(shape, lambda *_: (0,) * len(shape))


def params(grid=True, limit=24):
    return pltpu.CompilerParams(
        dimension_semantics=("arbitrary",) if grid else None, vmem_limit_bytes=limit << 20
    )


def cost(flops, moved):
    return pl.CostEstimate(flops=flops, bytes_accessed=moved, transcendentals=0)


SMEM = pl.BlockSpec(memory_space=pltpu.SMEM)
VMEM = pl.BlockSpec(memory_space=pltpu.VMEM)


HBM = pl.BlockSpec(memory_space=pltpu.HBM)


def in_vmem(array):
    return pltpu.with_memory_space_constraint(array, pltpu.VMEM)


def in_hbm(array):
    return pltpu.with_memory_space_constraint(array, pltpu.HBM)


def local(
    x_input, bc_input, z_gate, dt_input, conv_weight_x, conv_weight_bc, conv_bias_x, conv_bias_bc,
    dt_bias, decay_log, skip_scale, norm_gain,
):
    tokens, width = x_input.shape
    heads = dt_input.shape[0]
    blocks = tokens // SPAN
    seq = lax.axis_size("seq")
    tp = lax.axis_size("tp")
    bcw = bc_input.shape[1]
    half = width // 2
    cbx = conv_bias_x.reshape(1, width)
    cbbc = conv_bias_bc.reshape(1, bcw)
    gain = norm_gain.reshape(1, width)

    weight_arrays = (conv_weight_x, conv_weight_bc, cbx, cbbc)
    slab = pltpu.VMEM((width // 128 + 1, SPAN + 8, 128), F32)
    block_xw = pltpu.VMEM((SPAN, width), BF16)
    wide = pltpu.VMEM((tokens, width), BF16)
    narrow = pltpu.VMEM((tokens, STATE), BF16)
    state_shape = pltpu.VMEM((STATE, width), F32)
    x_near, bc_near, tail, xc, b_conv, w, cum, total, state = pl.pallas_call(
        first_kernel,
        in_specs=[HBM] * 9,
        out_specs=[VMEM] * 9,
        out_shape=[
            wide, pltpu.VMEM((tokens, bcw), BF16),
            pltpu.VMEM((8, width + bcw), BF16), wide, narrow,
            pltpu.VMEM((2 * heads, tokens), BF16), pltpu.VMEM((heads, tokens), F32),
            pltpu.VMEM((8, width), F32), state_shape,
        ],
        scratch_shapes=[
            slab, block_xw, pltpu.VMEM((heads, tokens), BF16), pltpu.VMEM((1, heads), F32), pltpu.VMEM((1, heads), F32),
            pltpu.VMEM((4, width), BF16), pltpu.VMEM((4, bcw), BF16),
            pltpu.VMEM((1, width), F32), pltpu.VMEM((1, bcw), F32),
            pltpu.SemaphoreType.DMA((15,)),
        ],
        compiler_params=params(False, 16),
        cost_estimate=cost(5_000_000_000, 4 << 20),
        name="first",
    )(
        *(
            in_hbm(each)
            for each in (
                x_input, bc_input, dt_input, dt_bias.reshape(1, heads),
                decay_log.reshape(1, heads), *weight_arrays,
            )
        )
    )
    halo = lax.ppermute(tail, "seq", [(k, k + 1) for k in range(seq - 1)])

    xc, b_conv, state = pl.pallas_call(
        later_kernel,
        in_specs=[VMEM] * 11,
        out_specs=[VMEM] * 3,
        out_shape=[wide, narrow, state_shape],
        scratch_shapes=[
            pltpu.VMEM((2, width // 128 + 1, SPAN + 8, 128), F32), pltpu.VMEM((2, SPAN, width), BF16)
        ],
        input_output_aliases={8: 2, 9: 0, 10: 1},
        compiler_params=params(False, 16),
        cost_estimate=cost(10_000_000_000, 4 << 20),
        name="later",
    )(x_near, bc_near, *weight_arrays, w, total, state, xc, b_conv)

    xc, b_conv, message = pl.pallas_call(
        second_kernel,
        in_specs=[VMEM] * 12,
        out_specs=[VMEM] * 3,
        out_shape=[wide, narrow, pltpu.VMEM((2 * STATE, half + 128), BF16)],
        scratch_shapes=[slab, block_xw],
        input_output_aliases={10: 0, 11: 1},
        compiler_params=params(False, 16),
        cost_estimate=cost(5_000_000_000, 4 << 20),
        name="second",
    )(x_near, bc_near, halo, *weight_arrays, w, total, state, xc, b_conv)

    sent = lax.all_to_all(message, "seq", 0, 0, tiled=True)

    y, c_conv = pl.pallas_call(
        middle_kernel,
        in_specs=[VMEM] * 9 + [SMEM],
        out_specs=[HBM, HBM],
        out_shape=[pltpu.HBM((tokens, width), F32), pltpu.HBM((tokens, STATE), BF16)],
        scratch_shapes=[
            state_shape, block_xw, pltpu.VMEM((tokens, width), F32),
            pltpu.VMEM((1, SPAN + 8, 128), F32), narrow,
            pltpu.SemaphoreType.DMA((tokens // SPAN + 1,)),
        ],
        compiler_params=params(False, 24),
        cost_estimate=cost(20_000_000_000, 10 << 20),
        name="middle",
    )(xc, b_conv, bc_input, halo, conv_weight_bc, cbbc, w, cum, total, skip_scale)

    starts = pl.pallas_call(
        prefix_kernel,
        in_specs=[VMEM, HBM],
        out_specs=VMEM,
        out_shape=pltpu.VMEM((2 * STATE, half), BF16),
        compiler_params=params(False, 4),
        cost_estimate=cost(2_000_000_000, 1 << 20),
        name="prefix",
    )(sent, in_hbm(y))
    mine = lax.all_to_all(starts, "seq", 0, 0, tiled=True)

    gated, sums = pl.pallas_call(
        gate_kernel,
        in_specs=[VMEM] * 5,
        out_specs=[VMEM] * 2,
        out_shape=[
            jax.ShapeDtypeStruct((tokens, width), F32), jax.ShapeDtypeStruct((tp, tokens), F32)
        ],
        scratch_shapes=[pltpu.VMEM((STATE, width), BF16)],
        compiler_params=params(False, 16),
        cost_estimate=cost(10_000_000_000, 10 << 20),
        name="gate",
    )(mine, in_vmem(c_conv), cum, in_vmem(y), in_vmem(z_gate))

    all_sums = lax.all_to_all(sums, "tp", 0, 0, tiled=True)

    return pl.pallas_call(
        scale_kernel,
        in_specs=[VMEM] * 3,
        out_specs=HBM,
        out_shape=pltpu.HBM((tokens, width), BF16),
        scratch_shapes=[
            pltpu.VMEM((tokens, width), BF16), pltpu.SemaphoreType.DMA((tokens // 128,))
        ],
        compiler_params=params(False, 16),
        cost_estimate=cost(5_000_000_000, 6 << 20),
        name="scale",
    )(gated, all_sums, gain)


def solution(mesh):
    return jax.shard_map(
        local,
        mesh=mesh,
        in_specs=(
            P("seq", "tp"), P("seq", "tp"), P("seq", "tp"), P("tp", "seq"),
            P(None, "tp"), P(None, "tp"),
            P("tp"), P("tp"), P("tp"), P("tp"), P("tp"), P("tp"),
        ),
        out_specs=P("seq", "tp"),
        check_vma=False,
    )
```
